32 devices in a mesh: dp: 1 (over z), tp: 4 (over y), pp: 8 (over x, core).
Axes of the slice: x: 4, y: 4, z: 1, core: 2. Of those that a mesh axis runs over, the one named last changes fastest.
The devices are a block of a 4x4x8 slice.
Arguments:
- x_in: bfloat16 [2, 6, 256, 2048], P(None, 'dp', 'tp')
- ln_params: float32 [8, 4, 2048], P('pp')
- w_q: bfloat16 [8, 2048, 16, 1, 128], P('pp', None, 'tp')
- w_k: bfloat16 [8, 2048, 16, 128], P('pp', None, 'tp')
- w_v: bfloat16 [8, 2048, 16, 128], P('pp', None, 'tp')
- w_o: bfloat16 [8, 16, 1, 128, 2048], P('pp', 'tp')
- w_up: bfloat16 [8, 2048, 8192], P('pp', None, 'tp')
- w_down: bfloat16 [8, 8192, 2048], P('pp', 'tp')
Outputs:
- output: bfloat16 [8, 2, 6, 256, 2048], P('pp', None, 'dp', 'tp')
All inputs are finite; a program needn't handle non-finite values.
Results may differ from the reference program's by a relative error of at most 0.0196532.
Values are sent between devices in bfloat16 or wider.
A program may use at most 768 MiB of HBM per device.

```python
import jax
import jax.numpy as jnp
from jax import lax

STAGES = 8
MICRO_BATCHES = 2
BATCH_SIZE = 6
SEQ_LEN = 256
D_MODEL = 2048
NUM_HEADS = 16
KV_COUNT = 16
HEAD_DIM = 128
FF_DIM = 8192

GROUP_SIZE = NUM_HEADS // KV_COUNT
LN_EPS = 1e-5
ROPE_BASE = 10000.0


def setup_inputs(seed: int = 0, part: int = 0) -> dict:
    rng_keys = jax.random.split(jax.random.key(seed), 8)
    x_key = jax.random.fold_in(rng_keys[0], part)
    x_in = jax.random.normal(x_key, (MICRO_BATCHES, BATCH_SIZE, SEQ_LEN, D_MODEL), jnp.float32)
    ln_offset = jnp.array([1.0, 0.0, 1.0, 0.0], jnp.float32)[None, :, None]
    ln_params = ln_offset + 0.5 * jax.random.normal(rng_keys[1], (STAGES, 4, D_MODEL), jnp.float32)
    in_scale = D_MODEL ** -0.5
    w_q = (1.25 * in_scale) * jax.random.normal(rng_keys[2], (STAGES, D_MODEL, KV_COUNT, GROUP_SIZE, HEAD_DIM), jnp.float32)
    w_k = (1.25 * in_scale) * jax.random.normal(rng_keys[3], (STAGES, D_MODEL, KV_COUNT, HEAD_DIM), jnp.float32)
    w_v = in_scale * jax.random.normal(rng_keys[4], (STAGES, D_MODEL, KV_COUNT, HEAD_DIM), jnp.float32)
    w_o = (3.0 * (NUM_HEADS * HEAD_DIM) ** -0.5) * jax.random.normal(rng_keys[5], (STAGES, KV_COUNT, GROUP_SIZE, HEAD_DIM, D_MODEL), jnp.float32)
    w_up = in_scale * jax.random.normal(rng_keys[6], (STAGES, D_MODEL, FF_DIM), jnp.float32)
    w_down = (FF_DIM ** -0.5) * jax.random.normal(rng_keys[7], (STAGES, FF_DIM, D_MODEL), jnp.float32)
    return {"x_in": x_in.astype(jnp.bfloat16), "ln_params": ln_params, "w_q": w_q.astype(jnp.bfloat16), "w_k": w_k.astype(jnp.bfloat16), "w_v": w_v.astype(jnp.bfloat16), "w_o": w_o.astype(jnp.bfloat16), "w_up": w_up.astype(jnp.bfloat16), "w_down": w_down.astype(jnp.bfloat16)}


def layer_norm(x_act, ln_gain, ln_bias):
    x_f32 = x_act.astype(jnp.float32)
    row_mean = jnp.mean(x_f32, axis=-1, keepdims=True)
    centred = x_f32 - row_mean
    variance = jnp.mean(centred * centred, axis=-1, keepdims=True)
    return (centred * lax.rsqrt(variance + LN_EPS) * ln_gain + ln_bias).astype(jnp.bfloat16)


def rope_tables():
    positions = jnp.arange(SEQ_LEN, dtype=jnp.float32)
    inv_freq = ROPE_BASE ** (-2.0 * jnp.arange(HEAD_DIM // 2, dtype=jnp.float32) / HEAD_DIM)
    angles = positions[:, None] * inv_freq[None, :]
    return jnp.cos(angles), jnp.sin(angles)


def apply_rope(proj, cos_tab, sin_tab):
    half_dim = HEAD_DIM // 2
    table_shape = (1, SEQ_LEN) + (1,) * (proj.ndim - 3) + (half_dim,)
    cos_bcast = cos_tab.reshape(table_shape)
    sin_bcast = sin_tab.reshape(table_shape)
    first_half = proj[..., :half_dim]
    second_half = proj[..., half_dim:]
    return jnp.concatenate([first_half * cos_bcast - second_half * sin_bcast, second_half * cos_bcast + first_half * sin_bcast], axis=-1)


def parallel_block(x_act, ln_par, w_q, w_k, w_v, w_o, w_up, w_down):
    num_rows = BATCH_SIZE * SEQ_LEN
    h_attn = layer_norm(x_act, ln_par[0], ln_par[1]).reshape(num_rows, D_MODEL)
    h_mlp = layer_norm(x_act, ln_par[2], ln_par[3]).reshape(num_rows, D_MODEL)
    cos_tab, sin_tab = rope_tables()
    q_proj = jnp.dot(h_attn, w_q.reshape(D_MODEL, NUM_HEADS * HEAD_DIM), preferred_element_type=jnp.float32)
    q_proj = apply_rope(q_proj.reshape(BATCH_SIZE, SEQ_LEN, KV_COUNT, GROUP_SIZE, HEAD_DIM), cos_tab, sin_tab).astype(jnp.bfloat16)
    k_proj = jnp.dot(h_attn, w_k.reshape(D_MODEL, KV_COUNT * HEAD_DIM), preferred_element_type=jnp.float32)
    k_proj = apply_rope(k_proj.reshape(BATCH_SIZE, SEQ_LEN, KV_COUNT, HEAD_DIM), cos_tab, sin_tab).astype(jnp.bfloat16)
    v_proj = jnp.dot(h_attn, w_v.reshape(D_MODEL, KV_COUNT * HEAD_DIM), preferred_element_type=jnp.float32).astype(jnp.bfloat16)
    v_proj = v_proj.reshape(BATCH_SIZE, SEQ_LEN, KV_COUNT, HEAD_DIM)
    allowed = jnp.arange(SEQ_LEN)[:, None, None] >= jnp.arange(SEQ_LEN)[None, None, :]

    def group_attention(operands):
        q_grp, k_grp, v_grp = operands
        scores = jnp.einsum("btgh,bsh->btgs", q_grp.astype(jnp.float32), k_grp.astype(jnp.float32)) * (HEAD_DIM ** -0.5)
        probs_bf = jax.nn.softmax(jnp.where(allowed, scores, -1e30), axis=-1).astype(jnp.bfloat16)
        return jnp.einsum("btgs,bsh->btgh", probs_bf.astype(jnp.float32), v_grp.astype(jnp.float32)).astype(jnp.bfloat16)

    context = lax.map(group_attention, (jnp.moveaxis(q_proj, 2, 0), jnp.moveaxis(k_proj, 2, 0), jnp.moveaxis(v_proj, 2, 0)))
    context = jnp.moveaxis(context, 0, 2).reshape(num_rows, NUM_HEADS * HEAD_DIM)
    attn_out = jnp.dot(context, w_o.reshape(NUM_HEADS * HEAD_DIM, D_MODEL), preferred_element_type=jnp.float32)
    hidden = jax.nn.gelu(jnp.dot(h_mlp, w_up, preferred_element_type=jnp.float32), approximate=False).astype(jnp.bfloat16)
    mlp_out = jnp.dot(hidden, w_down, preferred_element_type=jnp.float32)
    summed = x_act.reshape(num_rows, D_MODEL).astype(jnp.float32) + attn_out + mlp_out
    return summed.astype(jnp.bfloat16).reshape(BATCH_SIZE, SEQ_LEN, D_MODEL)


def reference(x_in, ln_params, w_q, w_k, w_v, w_o, w_up, w_down):
    def one_micro(x_act):
        def stage_step(x_cur, weights):
            ln_par, wq_s, wk_s, wv_s, wo_s, wup_s, wdown_s = weights
            y_next = parallel_block(x_cur, ln_par, wq_s, wk_s, wv_s, wo_s, wup_s, wdown_s)
            return y_next, y_next
        _, per_stage = lax.scan(stage_step, x_act, (ln_params, w_q, w_k, w_v, w_o, w_up, w_down))
        return per_stage
    stacked = lax.map(one_micro, x_in)
    return jnp.swapaxes(stacked, 0, 1)
```

```python
import functools

import jax
import jax.numpy as jnp
import numpy as np
from jax import lax
from jax.experimental import pallas as pl
from jax.experimental.pallas import tpu as pltpu
from jax.sharding import PartitionSpec as P

LN_EPS = 1e-5
ROPE_BASE = 10000.0
MESH = pl.DeviceIdType.MESH
F32 = jnp.float32
BF16 = jnp.bfloat16
COL_TILE = 512
LN_ROWS = 16


def rope_tables(seq_len, head_dim):
    positions = np.arange(seq_len, dtype=np.float32)
    inv_freq = np.float32(ROPE_BASE) ** (np.float32(-2.0) * np.arange(head_dim // 2, dtype=np.float32) / np.float32(head_dim))
    angles = positions[:, None] * inv_freq[None, :]
    cos_tab, sin_tab = np.cos(angles), np.sin(angles)
    return np.concatenate([cos_tab, cos_tab], axis=1), np.concatenate([-sin_tab, sin_tab], axis=1)


def pipeline_kernel(dims, x_in, ln_par, cos_ref, sin_ref, wqkv_hbm, wo_hbm, wup_hbm, wdn_hbm, out_ref,
                    wqkv, wo, wup, wdn, xbuf, yst, pst, rst, rel, fin, ha, hm, hid, qs, kc, vc, ctx,
                    w_sem, own_sem, nb_sem, op_sem, rel_sem, fin_sem, out_sem,
                    x0_send, f_send, wb_send, p_send, r_send, y_send, l_send):
    stages, rows, batch, seq_len, chunk, d_model, heads, hd, ff = dims
    blk = chunk // rows
    halves = seq_len // chunk
    num_chunks = x_in.shape[0] * batch * halves
    half = d_model // 2
    attn = heads * hd
    shard = seq_len // rows
    rows_per_half = rows // halves

    stage = lax.axis_index("pp")
    y = lax.axis_index("tp")
    up_y = lax.rem(y + 1, rows)
    dn_y = lax.rem(y + rows - 1, rows)
    op_y = lax.rem(y + 2, rows)
    first = stage == 0
    last = stage == stages - 1
    nxt = jnp.minimum(stage + 1, stages - 1)
    prv = jnp.maximum(stage - 1, 0)

    def block(row):
        return pl.ds(pl.multiple_of(row * blk, blk), blk)

    col_a, col_b = pl.ds(0, half), pl.ds(half, half)

    def rcopy(src, dst, send, recv, row, stg):
        return pltpu.make_async_remote_copy(src_ref=src, dst_ref=dst, send_sem=send, recv_sem=recv,
                                            device_id={"tp": row, "pp": stg}, device_id_type=MESH)

    weights = [pltpu.make_async_copy(src, dst, w_sem.at[i])
               for i, (src, dst) in enumerate(((wqkv_hbm, wqkv), (wup_hbm, wup), (wo_hbm, wo), (wdn_hbm, wdn)))]
    for copy in weights:
        copy.start()

    barrier = pltpu.get_barrier_semaphore()
    for shift in range(1, rows):
        pl.semaphore_signal(barrier, inc=1, device_id={"tp": lax.rem(y + shift, rows)}, device_id_type=MESH)

    @pl.when(jnp.logical_not(first))
    def _():
        for row in range(rows):
            pl.semaphore_signal(barrier, inc=1, device_id={"tp": row, "pp": prv}, device_id_type=MESH)

    @pl.when(jnp.logical_not(last))
    def _():
        for row in range(rows):
            pl.semaphore_signal(barrier, inc=1, device_id={"tp": row, "pp": nxt}, device_id_type=MESH)

    @pl.when(jnp.logical_or(first, last))
    def _():
        pl.semaphore_wait(barrier, 2 * rows - 1)

    @pl.when(jnp.logical_not(jnp.logical_or(first, last)))
    def _():
        pl.semaphore_wait(barrier, 3 * rows - 1)

    def seq_of(c):
        sigma = c // halves
        return sigma // batch, lax.rem(sigma, batch)

    my_part = lax.rem(y, rows_per_half)
    my_half = y // rows_per_half
    my_rows = pl.ds(pl.multiple_of(my_part * shard, shard), shard)

    def x0_copies(c):
        m, b = seq_of(c)
        slot = lax.rem(c // halves, 2)
        return [rcopy(x_in.at[m, b], xbuf.at[c, my_rows], x0_send.at[slot, i], own_sem.at[c],
                      lax.rem(y + 1 + i, rows), stage) for i in range(rows - 1)]

    def x0_issue(c):
        @pl.when(jnp.logical_and(first, my_half == lax.rem(c, halves)))
        def _():
            @pl.when(c >= 2 * halves)
            def _():
                for copy in x0_copies(c - 2 * halves):
                    copy.wait_send()
            for copy in x0_copies(c):
                copy.start()
            m, b = seq_of(c)
            pltpu.make_async_copy(x_in.at[m, b], xbuf.at[c, my_rows], own_sem.at[c]).start()

    def forwards(c):
        slot = lax.rem(c, 2)
        return [rcopy(xbuf.at[c, block(dn_y), col_a], xbuf.at[c, block(dn_y), col_a], f_send.at[slot, 0], op_sem.at[c], up_y, stage),
                rcopy(xbuf.at[c, block(up_y), col_b], xbuf.at[c, block(up_y), col_b], f_send.at[slot, 1], op_sem.at[c], dn_y, stage)]

    def wait_block(c, row, sem):
        ref = xbuf.at[c, block(row)]
        rcopy(ref, ref, f_send.at[0, 0], sem, up_y, stage).wait_recv()

    def relay_x(c):
        @pl.when(jnp.logical_not(first))
        def _():
            @pl.when(c >= 2)
            def _():
                for copy in forwards(c - 2):
                    copy.wait_send()
            fwd = forwards(c)
            wait_block(c, dn_y, nb_sem.at[c, 0])
            fwd[0].start()
            wait_block(c, up_y, nb_sem.at[c, 1])
            fwd[1].start()

    def wb_copy(c):
        m, b = seq_of(c)
        return rcopy(xbuf.at[c, my_rows], out_ref.at[0, m, b], wb_send.at[lax.rem(c // halves, 2)], out_sem.at[0], y, prv)

    def wait_x(c):
        @pl.when(first)
        def _():
            ref = xbuf.at[c]
            rcopy(ref, ref, f_send.at[0, 0], own_sem.at[c], up_y, stage).wait_recv()

        @pl.when(jnp.logical_not(first))
        def _():
            wait_block(c, y, own_sem.at[c])
            wait_block(c, op_y, op_sem.at[c])

            @pl.when(my_half == lax.rem(c, halves))
            def _():
                @pl.when(c >= 2 * halves)
                def _():
                    wb_copy(c - 2 * halves).wait_send()
                wb_copy(c).start()

    def p_copies(c):
        p = lax.rem(c, 2)
        return [rcopy(pst.at[p, block(op_y), col_a], rel.at[c, 0], p_send.at[p, 0], rel_sem.at[c, 0], dn_y, stage),
                rcopy(pst.at[p, block(up_y), col_a], fin.at[c, 1, :, col_a], p_send.at[p, 1], fin_sem.at[c], up_y, stage),
                rcopy(pst.at[p, block(op_y), col_b], rel.at[c, 1], p_send.at[p, 2], rel_sem.at[c, 1], up_y, stage),
                rcopy(pst.at[p, block(dn_y), col_b], fin.at[c, 0, :, col_b], p_send.at[p, 3], fin_sem.at[c], dn_y, stage)]

    def r_copies(c):
        p = lax.rem(c, 2)
        return [rcopy(rst.at[p, 0], fin.at[c, 0, :, col_a], r_send.at[p, 0], fin_sem.at[c], dn_y, stage),
                rcopy(rst.at[p, 1], fin.at[c, 1, :, col_b], r_send.at[p, 1], fin_sem.at[c], up_y, stage)]

    def relay_sums(c):
        p = lax.rem(c, 2)

        @pl.when(c >= 2)
        def _():
            for copy in r_copies(c - 2):
                copy.wait_send()
        out = r_copies(c)
        for i, (row, col) in enumerate(((dn_y, col_a), (up_y, col_b))):
            ref = rel.at[c, i]
            rcopy(ref, ref, r_send.at[0, i], rel_sem.at[c, i], up_y, stage).wait_recv()
            rst[p, i] = (rel[c, i].astype(F32) + pst[p, block(row), col].astype(F32)).astype(BF16)
            out[i].start()

    def y_copies(c):
        slot = lax.rem(c, 2)
        return [rcopy(yst.at[c], xbuf.at[c, block(y)], y_send.at[slot, 0], nb_sem.at[c, 0], up_y, nxt),
                rcopy(yst.at[c], xbuf.at[c, block(y)], y_send.at[slot, 1], nb_sem.at[c, 1], dn_y, nxt),
                rcopy(yst.at[c], xbuf.at[c, block(y)], y_send.at[slot, 2], own_sem.at[c], y, nxt)]

    def last_place(c):
        m, b = seq_of(c)
        token = lax.rem(c, halves) * chunk + y * blk
        row = token // shard
        start = pl.multiple_of(lax.rem(token, shard), blk)
        return row, out_ref.at[0, m, b, pl.ds(start, blk)]

    def last_copy(c):
        row, dst = last_place(c)
        return rcopy(yst.at[c], dst, l_send.at[lax.rem(c, 2)], out_sem.at[0], row, stage)

    def last_is_remote(c):
        return last_place(c)[0] != y

    def finish(c):
        p = lax.rem(c, 2)
        ref = fin.at[c]
        rcopy(ref, ref, r_send.at[0, 0], fin_sem.at[c], up_y, stage).wait_recv()
        total = xbuf[c, block(y)].astype(F32) + pst[p, block(y)].astype(F32)
        yst[c] = (total + fin[c, 0].astype(F32) + fin[c, 1].astype(F32)).astype(BF16)

        @pl.when(jnp.logical_not(last))
        def _():
            @pl.when(c >= 2)
            def _():
                for copy in y_copies(c - 2):
                    copy.wait_send()
            for copy in y_copies(c):
                copy.start()

        @pl.when(last)
        def _():
            @pl.when(jnp.logical_and(c >= 2, last_is_remote(c - 2)))
            def _():
                last_copy(c - 2).wait_send()

            @pl.when(last_is_remote(c))
            def _():
                last_copy(c).start()

            @pl.when(jnp.logical_not(last_is_remote(c)))
            def _():
                pltpu.make_async_copy(yst.at[c], last_place(c)[1], out_sem.at[0]).start()

    def norms(c):
        gain_a, bias_a = ln_par[0:1, :], ln_par[1:2, :]
        gain_m, bias_m = ln_par[2:3, :], ln_par[3:4, :]
        for start in range(0, chunk, LN_ROWS):
            part = pl.ds(start, LN_ROWS)
            x = xbuf[c, part].astype(F32)
            centred = x - jnp.mean(x, axis=-1, keepdims=True)
            scale = lax.rsqrt(jnp.mean(centred * centred, axis=-1, keepdims=True) + LN_EPS)
            normed = centred * scale
            ha[part] = (normed * gain_a + bias_a).astype(BF16)
            hm[part] = (normed * gain_m + bias_m).astype(BF16)

    def project(c):
        start = pl.multiple_of(lax.rem(c, halves) * chunk, chunk)
        where = pl.ds(start, chunk)
        cos, sin = cos_ref[where], sin_ref[where]

        def rope(val):
            turned = jnp.concatenate([val[:, hd // 2:], val[:, :hd // 2]], axis=1)
            return (val * cos + turned * sin).astype(BF16)

        h = ha[...]
        q = jnp.dot(h, wqkv[:, 0:attn], preferred_element_type=F32)
        for i in range(heads):
            qs[:, i * hd:(i + 1) * hd] = rope(q[:, i * hd:(i + 1) * hd])
        k = jnp.dot(h, wqkv[:, attn:2 * attn], preferred_element_type=F32)
        for i in range(heads):
            kc[where, i * hd:(i + 1) * hd] = rope(k[:, i * hd:(i + 1) * hd])
        vc[where, :] = jnp.dot(h, wqkv[:, 2 * attn:3 * attn], preferred_element_type=F32).astype(BF16)

    def attention(c):
        row_pos = lax.rem(c, halves) * chunk + lax.broadcasted_iota(jnp.int32, (chunk, seq_len), 0)
        allowed = row_pos >= lax.broadcasted_iota(jnp.int32, (chunk, seq_len), 1)
        for i in range(heads):
            cols = slice(i * hd, (i + 1) * hd)
            scores = lax.dot_general(qs[:, cols], kc[:, cols], (((1,), (1,)), ((), ())), preferred_element_type=F32) * (hd ** -0.5)
            scores = jnp.where(allowed, scores, -1e30)
            weights_ = jnp.exp(scores - jnp.max(scores, axis=-1, keepdims=True))
            probs = (weights_ / jnp.sum(weights_, axis=-1, keepdims=True)).astype(BF16)
            ctx[:, cols] = jnp.dot(probs, vc[:, cols], preferred_element_type=F32).astype(BF16)

    def mlp_up():
        h = hm[...]
        for start in range(0, ff, COL_TILE):
            cols = slice(start, start + COL_TILE)
            u = jnp.dot(h, wup[:, cols], preferred_element_type=F32)
            hid[:, cols] = (0.5 * u * (1.0 + lax.erf(u * np.float32(0.5 ** 0.5)))).astype(BF16)

    def down(c, begin, end):
        p = lax.rem(c, 2)
        a, h = ctx[...], hid[...]
        for start in range(begin, end, COL_TILE):
            cols = slice(start, start + COL_TILE)
            out = jnp.dot(a, wo[:, cols], preferred_element_type=F32) + jnp.dot(h, wdn[:, cols], preferred_element_type=F32)
            pst[p, :, cols] = out.astype(BF16)

    kc[...] = jnp.zeros_like(kc)
    vc[...] = jnp.zeros_like(vc)
    lead = min(3, num_chunks)
    for c in range(lead):
        x0_issue(jnp.int32(c))
    for copy in weights:
        copy.wait()

    def step(c, carry):
        relay_x(c)

        @pl.when(c + lead < num_chunks)
        def _():
            x0_issue(c + lead)
        wait_x(c)
        norms(c)
        project(c)

        @pl.when(c >= 1)
        def _():
            finish(c - 1)
        attention(c)
        mlp_up()

        @pl.when(c >= 2)
        def _():
            for copy in p_copies(c - 2):
                copy.wait_send()
        down(c, 0, half)
        sends = p_copies(c)
        sends[0].start()
        sends[1].start()
        down(c, half, d_model)
        sends[2].start()
        sends[3].start()
        relay_sums(c)
        return carry

    lax.fori_loop(0, num_chunks, step, 0)
    finish(jnp.int32(num_chunks - 1))

    for c in (num_chunks - 2, num_chunks - 1):
        c = jnp.int32(c)
        for copy in p_copies(c) + r_copies(c):
            copy.wait_send()

        @pl.when(jnp.logical_not(first))
        def _():
            for copy in forwards(c):
                copy.wait_send()

        @pl.when(jnp.logical_not(last))
        def _():
            for copy in y_copies(c):
                copy.wait_send()

        @pl.when(jnp.logical_and(last, last_is_remote(c)))
        def _():
            last_copy(c).wait_send()
    for back in (2, 1):
        c = num_chunks - back * halves + my_half

        @pl.when(first)
        def _():
            for copy in x0_copies(c):
                copy.wait_send()

        @pl.when(jnp.logical_not(first))
        def _():
            wb_copy(c).wait_send()
    whole = out_ref.at[0]
    rcopy(whole, whole, l_send.at[0], out_sem.at[0], up_y, stage).wait_recv()


def solution(mesh):
    stages, rows = mesh.shape["pp"], mesh.shape["tp"]

    def stage_body(x_in, ln_params, w_q, w_k, w_v, w_o, w_up, w_down):
        num_micro, batch, shard, d_model = x_in.shape
        heads, hd = w_k.shape[2:]
        ff = w_up.shape[2]
        attn = heads * hd
        seq_len = shard * rows
        chunk = seq_len // 2
        blk = chunk // rows
        halves = seq_len // chunk
        num_chunks = num_micro * batch * halves
        half = d_model // 2
        w_qkv = jnp.concatenate([w.reshape(d_model, attn) for w in (w_q, w_k, w_v)], axis=1)
        cos_tab, sin_tab = rope_tables(seq_len, hd)
        dims = (stages, rows, batch, seq_len, chunk, d_model, heads, hd, ff)
        hbm = pl.BlockSpec(memory_space=pl.ANY)
        vmem = pl.BlockSpec(memory_space=pltpu.VMEM)
        dma = pltpu.SemaphoreType.DMA
        return pl.pallas_call(
            functools.partial(pipeline_kernel, dims),
            out_shape=jax.ShapeDtypeStruct((1,) + x_in.shape, BF16),
            in_specs=[hbm, vmem, vmem, vmem, hbm, hbm, hbm, hbm],
            out_specs=hbm,
            scratch_shapes=[
                pltpu.VMEM((d_model, 3 * attn), BF16),
                pltpu.VMEM((attn, d_model), BF16),
                pltpu.VMEM((d_model, ff), BF16),
                pltpu.VMEM((ff, d_model), BF16),
                pltpu.VMEM((num_chunks, chunk, d_model), BF16),
                pltpu.VMEM((num_chunks, blk, d_model), BF16),
                pltpu.VMEM((2, chunk, d_model), BF16),
                pltpu.VMEM((2, 2, blk, half), BF16),
                pltpu.VMEM((num_chunks, 2, blk, half), BF16),
                pltpu.VMEM((num_chunks, 2, blk, d_model), BF16),
                pltpu.VMEM((chunk, d_model), BF16),
                pltpu.VMEM((chunk, d_model), BF16),
                pltpu.VMEM((chunk, ff), BF16),
                pltpu.VMEM((chunk, attn), BF16),
                pltpu.VMEM((seq_len, attn), BF16),
                pltpu.VMEM((seq_len, attn), BF16),
                pltpu.VMEM((chunk, attn), BF16),
                dma((4,)),
                dma((num_chunks,)),
                dma((num_chunks, 2)),
                dma((num_chunks,)),
                dma((num_chunks, 2)),
                dma((num_chunks,)),
                dma((1,)),
                dma((2, rows - 1)),
                dma((2, 2)),
                dma((2,)),
                dma((2, 4)),
                dma((2, 2)),
                dma((2, 3)),
                dma((2,)),
            ],
            compiler_params=pltpu.CompilerParams(collective_id=0, has_side_effects=True, vmem_limit_bytes=67_000_000),
        )(x_in, ln_params[0], cos_tab, sin_tab, w_qkv, w_o.reshape(attn, d_model), w_up[0], w_down[0])

    in_specs = (P(None, "dp", "tp", None), P("pp", None, None), P("pp", None, "tp", None, None), P("pp", None, "tp", None), P("pp", None, "tp", None), P("pp", "tp", None, None, None), P("pp", None, "tp"), P("pp", "tp", None))
    return jax.shard_map(stage_body, mesh=mesh, in_specs=in_specs, out_specs=P("pp", None, "dp", "tp", None), check_vma=False)
```

```python
import functools

import jax
import jax.numpy as jnp
import numpy as np
from jax import lax
from jax.experimental import pallas as pl
from jax.experimental.pallas import tpu as pltpu
from jax.sharding import PartitionSpec as P

LN_EPS = 1e-5
ROPE_BASE = 10000.0
MESH = pl.DeviceIdType.MESH
F32 = jnp.float32
BF16 = jnp.bfloat16
COL_TILE = 512
TILES = 2
HALVES = 2
SLOTS = 2
DIRECT = 8
ORDER = ("W", "N", "Q", "s-1", "t-1", "Z", "x-2o", "y-2o", "a", "b", "F-1", "G-1")
LN_ROWS = 16


def rope_tables(seq_len, head_dim):
    positions = np.arange(seq_len, dtype=np.float32)
    inv_freq = np.float32(ROPE_BASE) ** (np.float32(-2.0) * np.arange(head_dim // 2, dtype=np.float32) / np.float32(head_dim))
    angles = positions[:, None] * inv_freq[None, :]
    cos_tab, sin_tab = np.cos(angles), np.sin(angles)
    return np.concatenate([cos_tab, cos_tab], axis=1), np.concatenate([-sin_tab, sin_tab], axis=1)


def pipeline_kernel(dims, x_in, ln_par, cos_ref, sin_ref, wq_hbm, wk_hbm, wv_hbm, wo_hbm, wup_hbm, wdn_hbm, out_ref, gbuf,
                    wqkv, wup, wod, xbuf, yst, pst, sst, rec1, rec2, ha, hm, act, qs, kc, vc,
                    w_sem, x_sem, one_sem, two_sem, cr_sem, out_sem, x0_send, g_sem, g_send, wb_send, p_send, s_send, y_send, l_send, c_send):
    stages, rows, batch, seq_len, chunk, d_model, heads, hd, ff = dims
    halves = seq_len // chunk
    num_chunks = x_in.shape[0] * batch * halves
    seqs = num_chunks // halves
    half = d_model // 2
    tile = half // TILES
    attn = heads * hd
    shard = seq_len // rows
    per = rows // halves
    sb = chunk // 2

    stage = lax.axis_index("pp")
    y = lax.axis_index("tp")
    first = stage == 0
    last = stage == stages - 1
    nxt = jnp.minimum(stage + 1, stages - 1)
    prv = jnp.maximum(stage - 1, 0)
    others = [lax.rem(y + shift, rows) for shift in range(1, rows)]
    odd = lax.rem(stage, 2) == 1
    turning = jnp.logical_and(odd, jnp.logical_not(last))

    flip, mirror = y + 1 - 2 * lax.rem(y, 2), rows - 1 - y
    partner, cross = (flip, mirror), (mirror, flip)

    def share(row, k):
        return row // 2 if k == 0 else jnp.where(jnp.logical_or(row == 1, row == 2), 1, 0)

    def tokens(index):
        return pl.ds(pl.multiple_of(index * sb, sb), sb)

    def rows_of(row):
        return pl.ds(pl.multiple_of(row * shard, shard), shard)

    def within(row):
        return rows_of(lax.rem(row, per))

    col = (pl.ds(0, half), pl.ds(half, half))

    def rcopy(src, dst, send, recv, row, stg):
        return pltpu.make_async_remote_copy(src_ref=src, dst_ref=dst, send_sem=send, recv_sem=recv,
                                            device_id={"tp": row, "pp": stg}, device_id_type=MESH)

    def arrived(ref, sem):
        rcopy(ref, ref, sem, sem, others[0], stage).wait_recv()

    places = [(src, wqkv.at[:, pl.ds(i * attn, attn)]) for i, src in enumerate((wq_hbm, wk_hbm, wv_hbm))]
    places += [(wup_hbm, wup), (wo_hbm, wod.at[pl.ds(0, attn)]), (wdn_hbm, wod.at[pl.ds(attn, ff)])]
    weights = [pltpu.make_async_copy(src, dst, w_sem.at[i]) for i, (src, dst) in enumerate(places)]
    for copy in weights:
        copy.start()

    barrier = pltpu.get_barrier_semaphore()
    for row in others:
        pl.semaphore_signal(barrier, inc=1, device_id={"tp": row}, device_id_type=MESH)

    @pl.when(jnp.logical_not(first))
    def _():
        for row in range(rows):
            pl.semaphore_signal(barrier, inc=1, device_id={"tp": row, "pp": prv}, device_id_type=MESH)

    @pl.when(jnp.logical_not(last))
    def _():
        for row in range(rows):
            pl.semaphore_signal(barrier, inc=1, device_id={"tp": row, "pp": nxt}, device_id_type=MESH)

    @pl.when(jnp.logical_or(first, last))
    def _():
        pl.semaphore_signal(barrier, inc=1, device_id={"tp": y, "pp": jnp.where(first, stages - 1, 0)}, device_id_type=MESH)
        pl.semaphore_wait(barrier, 2 * rows)

    @pl.when(jnp.logical_not(jnp.logical_or(first, last)))
    def _():
        pl.semaphore_wait(barrier, 3 * rows - 1)

    def seq_of(c):
        sigma = c // halves
        return sigma // batch, lax.rem(sigma, batch)

    my_rows = within(y)

    def owns(c):
        return y // per == lax.rem(c, halves)

    def x0_local(c):
        m, b = seq_of(c)
        return pltpu.make_async_copy(x_in.at[m, b], xbuf.at[c, my_rows], x_sem.at[c])

    def x0_copies(c):
        m, b = seq_of(c)
        return [rcopy(x_in.at[m, b], xbuf.at[c, my_rows], x0_send.at[i], x_sem.at[c], row, stage) for i, row in enumerate(others)]

    def g_exchange(sigma):
        m, b = sigma // batch, sigma % batch
        return [rcopy(x_in.at[m, b], gbuf.at[sigma, rows_of(y)], g_send.at[0], g_sem.at[sigma], row, stage) for row in others]

    def g_pass(sigma):
        out = []
        for row in others:
            c = sigma * halves + row // per
            out.append(rcopy(gbuf.at[sigma, rows_of(row)], xbuf.at[c, within(row)], g_send.at[1], x_sem.at[c], y, 0))
        return out

    def feed():
        @pl.when(first)
        def _():
            for c in range(halves):
                @pl.when(owns(c))
                def _():
                    for copy in x0_copies(jnp.int32(c)):
                        copy.start()
            for c in range(num_chunks):
                @pl.when(owns(c))
                def _():
                    x0_local(jnp.int32(c)).start()

        @pl.when(last)
        def _():
            for sigma in range(1, seqs):
                for copy in g_exchange(sigma):
                    copy.start()
            for sigma in range(1, seqs):
                arrived(gbuf.at[sigma, pl.ds(0, seq_len - shard)], g_sem.at[sigma])
                for copy in g_pass(sigma):
                    copy.start()

    def wb_copy(c):
        m, b = seq_of(c)
        return rcopy(xbuf.at[c, my_rows], out_ref.at[0, m, b], wb_send.at[lax.rem(c // halves, 2)], out_sem.at[0], y, prv)

    def wait_x(c):
        arrived(xbuf.at[c], x_sem.at[c])

        @pl.when(jnp.logical_and(jnp.logical_not(first), owns(c)))
        def _():
            @pl.when(jnp.logical_and(c >= 2 * halves, jnp.logical_not(odd)))
            def _():
                wb_copy(c - 2 * halves).wait_send()
            wb_copy(c).start()

    def p_copies(c, k):
        p = lax.rem(c, SLOTS)
        out = []
        for i in range(TILES):
            cols = pl.ds(k * half + i * tile, tile)
            out.append(rcopy(pst.at[p, tokens(share(cross[k], k)), cols], rec1.at[c, k, :, pl.ds(i * tile, tile)],
                             p_send.at[p, k * TILES + i], one_sem.at[c, k], cross[k], stage))
        return out

    def s_copy(c, k):
        p = lax.rem(c, SLOTS)
        return rcopy(sst.at[p, k], rec2.at[c, k], s_send.at[p, k], two_sem.at[c, k], partner[k], stage)

    def first_sum(c, k):
        p = lax.rem(c, SLOTS)

        @pl.when(c >= SLOTS)
        def _():
            s_copy(c - SLOTS, k).wait_send()
        arrived(rec1.at[c, k], one_sem.at[c, k])
        own = pst[p, tokens(share(y, k)), col[k]]
        sst[p, k] = (rec1[c, k].astype(F32) + own.astype(F32)).astype(BF16)
        s_copy(c, k).start()

    def y_copies(c, k, around):
        p = lax.rem(c, SLOTS)
        where = (c, tokens(share(y, k)), col[k])
        side = rcopy(yst.at[p, k], xbuf.at[where], y_send.at[p, k, 0], cr_sem.at[c, k] if around else x_sem.at[c], cross[k], stage if around else nxt)
        return [side, rcopy(yst.at[p, k], xbuf.at[where], y_send.at[p, k, 1], x_sem.at[c], y, nxt)]

    def c_copy(c, k):
        ref = xbuf.at[c, tokens(share(cross[k], k)), col[k]]
        return rcopy(ref, ref, c_send.at[lax.rem(c, SLOTS), k], x_sem.at[c], y, nxt)

    def carry(c, k):
        @pl.when(jnp.logical_and(turning, c >= DIRECT))
        def _():
            @pl.when(c >= DIRECT + SLOTS)
            def _():
                c_copy(c - SLOTS, k).wait_send()
            arrived(xbuf.at[c, tokens(share(cross[k], k)), col[k]], cr_sem.at[c, k])
            c_copy(c, k).start()

    def last_place(c, k):
        token = lax.rem(c, halves) * chunk + share(y, k) * sb
        start = pl.multiple_of(lax.rem(token, shard), sb)
        m, b = seq_of(c)
        return token // shard, out_ref.at[0, m, b, pl.ds(start, sb), col[k]]

    def last_do(c, k, remote, local):
        p = lax.rem(c, SLOTS)
        row, dst = last_place(c, k)

        @pl.when(row == cross[k])
        def _():
            remote(rcopy(yst.at[p, k], dst, l_send.at[p, k], out_sem.at[k], cross[k], stage))

        @pl.when(row == y)
        def _():
            local(pltpu.make_async_copy(yst.at[p, k], dst, l_send.at[p, k]))

    def finish_half(c, k):
        p = lax.rem(c, SLOTS)

        @pl.when(jnp.logical_and(c >= SLOTS, jnp.logical_not(last)))
        def _():
            for copy in y_copies(c - SLOTS, k, False):
                copy.wait_send()

        @pl.when(jnp.logical_and(c >= SLOTS, last))
        def _():
            last_do(c - SLOTS, k, lambda copy: copy.wait_send(), lambda copy: copy.wait())
        arrived(rec2.at[c, k], two_sem.at[c, k])
        total = sst[p, k].astype(F32) + rec2[c, k].astype(F32)
        yst[p, k] = (xbuf[c, tokens(share(y, k)), col[k]].astype(F32) + total).astype(BF16)

        around = jnp.logical_and(turning, c >= DIRECT)

        @pl.when(around)
        def _():
            for copy in y_copies(c, k, True):
                copy.start()

        @pl.when(jnp.logical_not(jnp.logical_or(around, last)))
        def _():
            for copy in y_copies(c, k, False):
                copy.start()

        @pl.when(last)
        def _():
            last_do(c, k, lambda copy: copy.start(), lambda copy: copy.start())

    def norms(c):
        gain_a, bias_a = ln_par[0:1, :], ln_par[1:2, :]
        gain_m, bias_m = ln_par[2:3, :], ln_par[3:4, :]
        for start in range(0, chunk, LN_ROWS):
            part = pl.ds(start, LN_ROWS)
            x = xbuf[c, part].astype(F32)
            centred = x - jnp.mean(x, axis=-1, keepdims=True)
            scale = lax.rsqrt(jnp.mean(centred * centred, axis=-1, keepdims=True) + LN_EPS)
            normed = centred * scale
            ha[part] = (normed * gain_a + bias_a).astype(BF16)
            hm[part] = (normed * gain_m + bias_m).astype(BF16)

    def project(c):
        start = pl.multiple_of(lax.rem(c, halves) * chunk, chunk)
        where = pl.ds(start, chunk)
        cos, sin = cos_ref[where], sin_ref[where]

        def rope(val):
            turned = jnp.concatenate([val[:, hd // 2:], val[:, :hd // 2]], axis=1)
            return (val * cos + turned * sin).astype(BF16)

        h = ha[...]
        q = jnp.dot(h, wqkv[:, 0:attn], preferred_element_type=F32)
        for i in range(heads):
            qs[:, i * hd:(i + 1) * hd] = rope(q[:, i * hd:(i + 1) * hd])
        k = jnp.dot(h, wqkv[:, attn:2 * attn], preferred_element_type=F32)
        for i in range(heads):
            kc[where, i * hd:(i + 1) * hd] = rope(k[:, i * hd:(i + 1) * hd])
        vc[where, :] = jnp.dot(h, wqkv[:, 2 * attn:3 * attn], preferred_element_type=F32).astype(BF16)

    def attend(c, i):
        row_pos = lax.rem(c, halves) * chunk + lax.broadcasted_iota(jnp.int32, (chunk, seq_len), 0)
        allowed = row_pos >= lax.broadcasted_iota(jnp.int32, (chunk, seq_len), 1)
        cols = slice(i * hd, (i + 1) * hd)
        scores = lax.dot_general(qs[:, cols], kc[:, cols], (((1,), (1,)), ((), ())), preferred_element_type=F32) * (hd ** -0.5)
        scores = jnp.where(allowed, scores, -1e30)
        weights_ = jnp.exp(scores - jnp.max(scores, axis=-1, keepdims=True))
        return (weights_ / jnp.sum(weights_, axis=-1, keepdims=True)).astype(BF16)

    def contract(i, probs):
        cols = slice(i * hd, (i + 1) * hd)
        act[:, cols] = jnp.dot(probs, vc[:, cols], preferred_element_type=F32).astype(BF16)

    def attention(c):
        for i in range(heads):
            contract(i, attend(c, i))

    def up_tile(i, width):
        cols = slice(i * width, (i + 1) * width)
        u = jnp.dot(hm[...], wup[:, cols], preferred_element_type=F32)
        act[:, attn + i * width:attn + (i + 1) * width] = (0.5 * u * (1.0 + lax.erf(u * np.float32(0.5 ** 0.5)))).astype(BF16)

    def mlp_up():
        for i in range(ff // COL_TILE):
            up_tile(i, COL_TILE)

    def attention_and_up(c):
        for i in range(heads):
            probs = attend(c, i)
            up_tile(i, ff // heads)
            contract(i, probs)

    def down(c, k):
        p = lax.rem(c, SLOTS)
        a = act[...]
        copies = p_copies(c, k)
        for i, start in enumerate(range(k * half, (k + 1) * half, tile)):
            cols = slice(start, start + tile)
            out = jnp.dot(a, wod[:, cols], preferred_element_type=F32)
            pst[p, :, cols] = out.astype(BF16)
            copies[i].start()

    kc[...] = jnp.zeros_like(kc)
    vc[...] = jnp.zeros_like(vc)
    feed()

    def loaded(c, which):
        @pl.when(c == 0)
        def _():
            for copy in which:
                copy.wait()

    def project_first(c):
        loaded(c, weights[:3])
        project(c)

    def mlp_up_first(c):
        loaded(c, weights[3:4])
        mlp_up()

    def both(c):
        loaded(c, weights[3:4])
        attention_and_up(c)

    def down_a(c):
        loaded(c, weights[4:])

        @pl.when(c >= SLOTS)
        def _():
            for k in range(2):
                for copy in p_copies(c - SLOTS, k):
                    copy.wait_send()

        @pl.when(jnp.logical_and(odd, owns(c)))
        def _():
            wb_copy(c).wait_send()
        down(c, 0)

    acts = {"W": wait_x, "N": norms, "Q": project_first, "A": attention, "U": mlp_up_first, "Z": both, "a": down_a, "b": lambda c: down(c, 1),
            "s": lambda c: first_sum(c, 0), "t": lambda c: first_sum(c, 1), "x": lambda c: carry(c, 0), "y": lambda c: carry(c, 1), "F": lambda c: finish_half(c, 0), "G": lambda c: finish_half(c, 1)}
    order = [(o[0], int(o[1:].rstrip("eo") or 0), {"e": jnp.logical_not(odd), "o": odd}.get(o[-1])) for o in ORDER]

    def guarded(ok, fn, c):
        @pl.when(ok)
        def _():
            fn(c)

    def step(c, carry):
        for name, shift, which in order:
            fn = acts[name]
            if shift < 0:
                ok = c + shift >= 0
                guarded(ok if which is None else jnp.logical_and(ok, which), fn, c + shift)
            elif which is not None:
                guarded(which, fn, c)
            else:
                fn(c)
        return carry

    lax.fori_loop(0, num_chunks, step, 0)
    for c in range(num_chunks, num_chunks + max(-shift for _, shift, _ in order)):
        for name, shift, which in order:
            if shift < 0 and c + shift < num_chunks:
                if which is None:
                    acts[name](jnp.int32(c + shift))
                else:
                    guarded(which, acts[name], jnp.int32(c + shift))

    for c in range(num_chunks - SLOTS, num_chunks):
        c = jnp.int32(c)
        for k in range(2):
            for copy in p_copies(c, k) + [s_copy(c, k)]:
                copy.wait_send()

            @pl.when(jnp.logical_not(last))
            def _():
                for copy in y_copies(c, k, False):
                    copy.wait_send()

            @pl.when(turning)
            def _():
                c_copy(c, k).wait_send()

            @pl.when(last)
            def _():
                last_do(c, k, lambda copy: copy.wait_send(), lambda copy: copy.wait())
    for back in (2, 1):
        c = num_chunks - back * halves + y // per

        @pl.when(jnp.logical_not(jnp.logical_or(first, odd)))
        def _():
            wb_copy(c).wait_send()

    @pl.when(first)
    def _():
        for c in range(halves):
            @pl.when(owns(c))
            def _():
                for copy in x0_copies(jnp.int32(c)):
                    copy.wait_send()

    @pl.when(last)
    def _():
        for i in range(2):
            ref = gbuf.at[pl.ds(0, seqs - 1), pl.ds(0, seq_len - shard)]
            rcopy(ref, ref, g_send.at[i], g_send.at[i], others[0], stage).wait_send()
        for k in range(2):
            @pl.when(jnp.logical_or(per == 1, share(y, k) != lax.rem(y, per)))
            def _():
                arrived(out_ref.at[0, :, :, pl.ds(0, sb), col[k]], out_sem.at[k])

    @pl.when(jnp.logical_not(last))
    def _():
        arrived(out_ref.at[0], out_sem.at[0])


def solution(mesh):
    stages, rows = mesh.shape["pp"], mesh.shape["tp"]

    def stage_body(x_in, ln_params, w_q, w_k, w_v, w_o, w_up, w_down):
        num_micro, batch, shard, d_model = x_in.shape
        heads, hd = w_k.shape[2:]
        ff = w_up.shape[2]
        attn = heads * hd
        seq_len = shard * rows
        chunk = seq_len // HALVES
        num_chunks = num_micro * batch * HALVES
        sb = chunk // 2
        half = d_model // 2
        w_qkv = [w.reshape(d_model, attn) for w in (w_q, w_k, w_v)]
        cos_tab, sin_tab = rope_tables(seq_len, hd)
        dims = (stages, rows, batch, seq_len, chunk, d_model, heads, hd, ff)
        hbm = pl.BlockSpec(memory_space=pl.ANY)
        vmem = pl.BlockSpec(memory_space=pltpu.VMEM)
        dma = pltpu.SemaphoreType.DMA
        return pl.pallas_call(
            functools.partial(pipeline_kernel, dims),
            out_shape=(jax.ShapeDtypeStruct((1,) + x_in.shape, BF16), jax.ShapeDtypeStruct((num_micro * batch, seq_len, d_model), BF16)),
            in_specs=[hbm, vmem, vmem, vmem] + [hbm] * 6,
            out_specs=(hbm, hbm),
            scratch_shapes=[
                pltpu.VMEM((d_model, 3 * attn), BF16),
                pltpu.VMEM((d_model, ff), BF16),
                pltpu.VMEM((attn + ff, d_model), BF16),
                pltpu.VMEM((num_chunks, chunk, d_model), BF16),
                pltpu.VMEM((SLOTS, 2, sb, half), BF16),
                pltpu.VMEM((SLOTS, chunk, d_model), BF16),
                pltpu.VMEM((SLOTS, 2, sb, half), BF16),
                pltpu.VMEM((num_chunks, 2, sb, half), BF16),
                pltpu.VMEM((num_chunks, 2, sb, half), BF16),
                pltpu.VMEM((chunk, d_model), BF16),
                pltpu.VMEM((chunk, d_model), BF16),
                pltpu.VMEM((chunk, attn + ff), BF16),
                pltpu.VMEM((chunk, attn), BF16),
                pltpu.VMEM((seq_len, attn), BF16),
                pltpu.VMEM((seq_len, attn), BF16),
                dma((6,)),
                dma((num_chunks,)),
                dma((num_chunks, 2)),
                dma((num_chunks, 2)),
                dma((num_chunks, 2)),
                dma((2,)),
                dma((rows - 1,)),
                dma((num_micro * batch,)),
                dma((2,)),
                dma((2,)),
                dma((SLOTS, 2 * TILES)),
                dma((SLOTS, 2)),
                dma((SLOTS, 2, 2)),
                dma((SLOTS, 2)),
                dma((SLOTS, 2)),
            ],
            compiler_params=pltpu.CompilerParams(collective_id=0, has_side_effects=True, vmem_limit_bytes=67_000_000),
        )(x_in, ln_params[0], cos_tab, sin_tab, *w_qkv, w_o.reshape(attn, d_model), w_up[0], w_down[0])[0]

    in_specs = (P(None, "dp", "tp", None), P("pp", None, None), P("pp", None, "tp", None, None), P("pp", None, "tp", None), P("pp", None, "tp", None), P("pp", "tp", None, None, None), P("pp", None, "tp"), P("pp", "tp", None))
    return jax.shard_map(stage_body, mesh=mesh, in_specs=in_specs, out_specs=P("pp", None, "dp", "tp", None), check_vma=False)
```

```python
import functools

import jax
import jax.numpy as jnp
import numpy as np
from jax import lax
from jax.experimental import pallas as pl
from jax.experimental.pallas import tpu as pltpu
from jax.sharding import PartitionSpec as P

LN_EPS = 1e-5
ROPE_BASE = 10000.0
MESH = pl.DeviceIdType.MESH
F32 = jnp.float32
BF16 = jnp.bfloat16
COL_TILE = 512
TILES = 2
HALVES = 2
SLOTS = 2
DIRECT = 8
ORDER = ("W", "N", "s-1", "t-1", "Ye", "Zo", "ao", "x-2o", "y-2o", "b", "F-1", "G-1")
LN_ROWS = 16


def rope_tables(seq_len, head_dim):
    positions = np.arange(seq_len, dtype=np.float32)
    inv_freq = np.float32(ROPE_BASE) ** (np.float32(-2.0) * np.arange(head_dim // 2, dtype=np.float32) / np.float32(head_dim))
    angles = positions[:, None] * inv_freq[None, :]
    cos_tab, sin_tab = np.cos(angles), np.sin(angles)
    return np.concatenate([cos_tab, cos_tab], axis=1), np.concatenate([-sin_tab, sin_tab], axis=1)


def pipeline_kernel(dims, x_in, ln_par, cos_ref, sin_ref, wq_hbm, wk_hbm, wv_hbm, wo_hbm, wup_hbm, wdn_hbm, out_ref, gbuf,
                    raw, wqkv, wup, wod, xbuf, yst, pst, sst, rec1, rec2, ha, hm, stat, act, qs, kc, vc,
                    w_sem, x_sem, one_sem, two_sem, cr_sem, out_sem, x0_send, g_sem, g_send, wb_send, p_send, s_send, y_send, l_send, c_send):
    stages, rows, batch, seq_len, chunk, d_model, heads, hd, ff = dims
    halves = seq_len // chunk
    num_chunks = x_in.shape[0] * batch * halves
    seqs = num_chunks // halves
    half = d_model // 2
    tile = half // TILES
    attn = heads * hd
    shard = seq_len // rows
    per = rows // halves
    sb = chunk // 2

    stage = lax.axis_index("pp")
    y = lax.axis_index("tp")
    first = stage == 0
    last = stage == stages - 1
    nxt = jnp.minimum(stage + 1, stages - 1)
    prv = jnp.maximum(stage - 1, 0)
    others = [lax.rem(y + shift, rows) for shift in range(1, rows)]
    odd = lax.rem(stage, 2) == 1
    turning = jnp.logical_and(odd, jnp.logical_not(last))

    flip, mirror = y + 1 - 2 * lax.rem(y, 2), rows - 1 - y
    partner, cross = (flip, mirror), (mirror, flip)

    def share(row, k):
        return row // 2 if k == 0 else jnp.where(jnp.logical_or(row == 1, row == 2), 1, 0)

    def tokens(index):
        return pl.ds(pl.multiple_of(index * sb, sb), sb)

    def rows_of(row):
        return pl.ds(pl.multiple_of(row * shard, shard), shard)

    def within(row):
        return rows_of(lax.rem(row, per))

    col = (pl.ds(0, half), pl.ds(half, half))

    def rcopy(src, dst, send, recv, row, stg):
        return pltpu.make_async_remote_copy(src_ref=src, dst_ref=dst, send_sem=send, recv_sem=recv,
                                            device_id={"tp": row, "pp": stg}, device_id_type=MESH)

    def arrived(ref, sem):
        rcopy(ref, ref, sem, sem, others[0], stage).wait_recv()

    places = [(src, raw.at[i]) for i, src in enumerate((wq_hbm, wk_hbm, wv_hbm))]
    places += [(wup_hbm, wup), (wo_hbm, wod.at[pl.ds(0, attn)]), (wdn_hbm, wod.at[pl.ds(attn, ff)])]
    weights = [pltpu.make_async_copy(src, dst, w_sem.at[i]) for i, (src, dst) in enumerate(places)]
    for copy in weights:
        copy.start()

    barrier = pltpu.get_barrier_semaphore()
    for row in others:
        pl.semaphore_signal(barrier, inc=1, device_id={"tp": row}, device_id_type=MESH)

    @pl.when(jnp.logical_not(first))
    def _():
        for row in range(rows):
            pl.semaphore_signal(barrier, inc=1, device_id={"tp": row, "pp": prv}, device_id_type=MESH)

    @pl.when(jnp.logical_not(last))
    def _():
        for row in range(rows):
            pl.semaphore_signal(barrier, inc=1, device_id={"tp": row, "pp": nxt}, device_id_type=MESH)

    @pl.when(jnp.logical_or(first, last))
    def _():
        pl.semaphore_signal(barrier, inc=1, device_id={"tp": y, "pp": jnp.where(first, stages - 1, 0)}, device_id_type=MESH)
        pl.semaphore_wait(barrier, 2 * rows)

    @pl.when(jnp.logical_not(jnp.logical_or(first, last)))
    def _():
        pl.semaphore_wait(barrier, 3 * rows - 1)

    def seq_of(c):
        sigma = c // halves
        return sigma // batch, lax.rem(sigma, batch)

    my_rows = within(y)

    def owns(c):
        return y // per == lax.rem(c, halves)

    def x0_local(c):
        m, b = seq_of(c)
        return pltpu.make_async_copy(x_in.at[m, b], xbuf.at[c, my_rows], x_sem.at[c])

    def x0_copies(c):
        m, b = seq_of(c)
        return [rcopy(x_in.at[m, b], xbuf.at[c, my_rows], x0_send.at[i], x_sem.at[c], row, stage) for i, row in enumerate(others)]

    def g_exchange(sigma):
        m, b = sigma // batch, sigma % batch
        return [rcopy(x_in.at[m, b], gbuf.at[sigma, rows_of(y)], g_send.at[0], g_sem.at[sigma], row, stage) for row in others]

    def g_pass(sigma):
        out = []
        for row in others:
            c = sigma * halves + row // per
            out.append(rcopy(gbuf.at[sigma, rows_of(row)], xbuf.at[c, within(row)], g_send.at[1], x_sem.at[c], y, 0))
        return out

    def x0_start(c):
        @pl.when(owns(c))
        def _():
            for copy in x0_copies(jnp.int32(c)):
                copy.start()

    def feed():
        @pl.when(first)
        def _():
            x0_start(0)
            for c in range(num_chunks):
                @pl.when(owns(c))
                def _():
                    x0_local(jnp.int32(c)).start()

        @pl.when(last)
        def _():
            for sigma in range(1, seqs):
                for copy in g_exchange(sigma):
                    copy.start()

    def pass_on():
        @pl.when(last)
        def _():
            for sigma in range(1, seqs):
                arrived(gbuf.at[sigma, pl.ds(0, seq_len - shard)], g_sem.at[sigma])
                for copy in g_pass(sigma):
                    copy.start()

    def wb_copy(c):
        m, b = seq_of(c)
        return rcopy(xbuf.at[c, my_rows], out_ref.at[0, m, b], wb_send.at[lax.rem(c // halves, 2)], out_sem.at[0], y, prv)

    def wait_x(c):
        arrived(xbuf.at[c], x_sem.at[c])

        @pl.when(jnp.logical_and(jnp.logical_not(first), owns(c)))
        def _():
            @pl.when(jnp.logical_and(c >= 2 * halves, jnp.logical_not(odd)))
            def _():
                wb_copy(c - 2 * halves).wait_send()
            wb_copy(c).start()

    def piece(k, i):
        return pl.ds(k * half + i * tile, tile)

    def p_copy(c, k, i):
        p = lax.rem(c, SLOTS)
        return rcopy(pst.at[p, tokens(share(cross[k], k)), piece(k, i)], rec1.at[c, k, :, piece(0, i)],
                     p_send.at[p, k, i], one_sem.at[c, k], cross[k], stage)

    def s_copy(c, k, i):
        p = lax.rem(c, SLOTS)
        return rcopy(sst.at[p, k, :, piece(0, i)], rec2.at[c, k, :, piece(0, i)], s_send.at[p, k, i], two_sem.at[c, k, i], partner[k], stage)

    def first_sum(c, k):
        p = lax.rem(c, SLOTS)

        @pl.when(c >= SLOTS)
        def _():
            for i in range(TILES):
                s_copy(c - SLOTS, k, i).wait_send()
        arrived(rec1.at[c, k], one_sem.at[c, k])
        own = pst[p, tokens(share(y, k)), col[k]]
        sst[p, k] = (rec1[c, k].astype(F32) + own.astype(F32)).astype(BF16)
        for i in range(TILES):
            s_copy(c, k, i).start()

    def y_copies(c, k, i, around):
        p = lax.rem(c, SLOTS)
        src, where = yst.at[p, k, :, piece(0, i)], (c, tokens(share(y, k)), piece(k, i))
        side = rcopy(src, xbuf.at[where], y_send.at[p, k, i, 0], cr_sem.at[c, k] if around else x_sem.at[c], cross[k], stage if around else nxt)
        return [side, rcopy(src, xbuf.at[where], y_send.at[p, k, i, 1], x_sem.at[c], y, nxt)]

    def c_copy(c, k):
        ref = xbuf.at[c, tokens(share(cross[k], k)), col[k]]
        return rcopy(ref, ref, c_send.at[lax.rem(c, SLOTS), k], x_sem.at[c], y, nxt)

    def carry(c, k):
        @pl.when(jnp.logical_and(turning, c >= DIRECT))
        def _():
            @pl.when(c >= DIRECT + SLOTS)
            def _():
                c_copy(c - SLOTS, k).wait_send()
            arrived(xbuf.at[c, tokens(share(cross[k], k)), col[k]], cr_sem.at[c, k])
            c_copy(c, k).start()

    def last_place(c, k, i):
        token = lax.rem(c, halves) * chunk + share(y, k) * sb
        start = pl.multiple_of(lax.rem(token, shard), sb)
        m, b = seq_of(c)
        return token // shard, out_ref.at[0, m, b, pl.ds(start, sb), piece(k, i)]

    def last_do(c, k, i, remote, local):
        p = lax.rem(c, SLOTS)
        row, dst = last_place(c, k, i)
        src, sem = yst.at[p, k, :, piece(0, i)], l_send.at[p, k, i]

        @pl.when(row == cross[k])
        def _():
            remote(rcopy(src, dst, sem, out_sem.at[k], cross[k], stage))

        @pl.when(row == y)
        def _():
            local(pltpu.make_async_copy(src, dst, sem))

    def finish(c, i):
        p = lax.rem(c, SLOTS)
        around = jnp.logical_and(turning, c >= DIRECT)
        for k in range(2):
            @pl.when(jnp.logical_and(c >= SLOTS, jnp.logical_not(last)))
            def _():
                for copy in y_copies(c - SLOTS, k, i, False):
                    copy.wait_send()

            @pl.when(jnp.logical_and(c >= SLOTS, last))
            def _():
                last_do(c - SLOTS, k, i, lambda copy: copy.wait_send(), lambda copy: copy.wait())
            arrived(rec2.at[c, k, :, piece(0, i)], two_sem.at[c, k, i])
            total = sst[p, k, :, piece(0, i)].astype(F32) + rec2[c, k, :, piece(0, i)].astype(F32)
            yst[p, k, :, piece(0, i)] = (xbuf[c, tokens(share(y, k)), piece(k, i)].astype(F32) + total).astype(BF16)

            @pl.when(around)
            def _():
                for copy in y_copies(c, k, i, True):
                    copy.start()

            @pl.when(jnp.logical_not(jnp.logical_or(around, last)))
            def _():
                for copy in y_copies(c, k, i, False):
                    copy.start()

            @pl.when(last)
            def _():
                last_do(c, k, i, lambda copy: copy.start(), lambda copy: copy.start())

    lanes = stat.shape[2]

    def norms(c):
        gain, bias = ln_par[0:1, :], ln_par[1:2, :]
        for start in range(0, chunk, LN_ROWS):
            part = pl.ds(start, LN_ROWS)
            x = xbuf[c, part].astype(F32)
            mean = jnp.mean(x, axis=-1, keepdims=True)
            centred = x - mean
            scale = lax.rsqrt(jnp.mean(centred * centred, axis=-1, keepdims=True) + LN_EPS)
            ha[part] = (centred * scale * gain + bias).astype(BF16)
            stat[0, part] = jnp.broadcast_to(mean, (LN_ROWS, lanes))
            stat[1, part] = jnp.broadcast_to(scale, (LN_ROWS, lanes))

    def second_norms(c, begin, end):
        for start in range(begin, end, LN_ROWS):
            part = pl.ds(start, LN_ROWS)
            mean, scale = stat[0, part], stat[1, part]
            for left in range(0, d_model, lanes):
                cols = slice(left, left + lanes)
                hm[part, cols] = ((xbuf[c, part, cols].astype(F32) - mean) * scale * ln_par[2:3, cols] + ln_par[3:4, cols]).astype(BF16)

    def project(c):
        start = pl.multiple_of(lax.rem(c, halves) * chunk, chunk)
        where = pl.ds(start, chunk)
        cos, sin = cos_ref[where], sin_ref[where]

        def rope(val):
            turned = jnp.concatenate([val[:, hd // 2:], val[:, :hd // 2]], axis=1)
            return (val * cos + turned * sin).astype(BF16)

        h = ha[...]
        q = jnp.dot(h, wqkv[:, 0:attn], preferred_element_type=F32)
        for i in range(heads):
            qs[:, i * hd:(i + 1) * hd] = rope(q[:, i * hd:(i + 1) * hd])
        second_norms(c, 0, chunk // 2)
        k = jnp.dot(h, wqkv[:, attn:2 * attn], preferred_element_type=F32)
        for i in range(heads):
            kc[where, i * hd:(i + 1) * hd] = rope(k[:, i * hd:(i + 1) * hd])
        second_norms(c, chunk // 2, chunk)
        vc[where, :] = jnp.dot(h, wqkv[:, 2 * attn:3 * attn], preferred_element_type=F32).astype(BF16)

    def attend(c, i):
        row_pos = lax.rem(c, halves) * chunk + lax.broadcasted_iota(jnp.int32, (chunk, seq_len), 0)
        allowed = row_pos >= lax.broadcasted_iota(jnp.int32, (chunk, seq_len), 1)
        cols = slice(i * hd, (i + 1) * hd)
        scores = lax.dot_general(qs[:, cols], kc[:, cols], (((1,), (1,)), ((), ())), preferred_element_type=F32) * (hd ** -0.5)
        scores = jnp.where(allowed, scores, -1e30)
        weights_ = jnp.exp(scores - jnp.max(scores, axis=-1, keepdims=True))
        return (weights_ / jnp.sum(weights_, axis=-1, keepdims=True)).astype(BF16)

    def contract(i, probs):
        cols = slice(i * hd, (i + 1) * hd)
        act[:, cols] = jnp.dot(probs, vc[:, cols], preferred_element_type=F32).astype(BF16)

    def up_tile(i, width):
        cols = slice(i * width, (i + 1) * width)
        u = jnp.dot(hm[...], wup[:, cols], preferred_element_type=F32)
        act[:, attn + i * width:attn + (i + 1) * width] = (0.5 * u * (1.0 + lax.erf(u * np.float32(0.5 ** 0.5)))).astype(BF16)

    def attention_and_up(c):
        for i in range(heads):
            probs = attend(c, i)
            up_tile(i, ff // heads)
            contract(i, probs)

    def down(c, i):
        p = lax.rem(c, SLOTS)
        a = act[...]
        for k in range(2):
            cols = slice(k * half + i * tile, k * half + (i + 1) * tile)
            pst[p, :, cols] = jnp.dot(a, wod[:, cols], preferred_element_type=F32).astype(BF16)
        for k in range(2):
            p_copy(c, k, i).start()

    kc[...] = jnp.zeros_like(kc)
    vc[...] = jnp.zeros_like(vc)
    feed()

    depth = hd // 2
    group = depth * heads
    out_row, in_row = (lax.broadcasted_iota(jnp.int32, (group, group), axis) for axis in (0, 1))
    pick = (in_row == heads * lax.rem(out_row, depth) + out_row // depth).astype(F32).astype(BF16)
    for copy in weights[:3]:
        copy.wait()

    def sort_heads(j, carry):
        rows_in = pl.ds(pl.multiple_of(j * group, group), group)
        rows_out = pl.ds(pl.multiple_of(j * depth, depth), depth)
        pair = jnp.dot(pick, jnp.concatenate([raw[0, rows_in], raw[1, rows_in]], axis=1), preferred_element_type=F32).astype(BF16)
        alone = jnp.dot(pick, raw[2, rows_in], preferred_element_type=F32).astype(BF16)
        for i, val in enumerate((pair[:, :hd], pair[:, hd:], alone)):
            for h in range(heads):
                wqkv[rows_out, i * attn + h * hd:i * attn + (h + 1) * hd] = val[h * depth:(h + 1) * depth]
        return carry

    lax.fori_loop(0, d_model // depth, sort_heads, 0, unroll=4)
    @pl.when(first)
    def _():
        for c in range(1, halves):
            x0_start(c)
    pass_on()
    for copy in weights[3:]:
        copy.wait()

    def free_sums(c):
        @pl.when(c >= SLOTS)
        def _():
            for k in range(2):
                for i in range(TILES):
                    p_copy(c - SLOTS, k, i).wait_send()

        @pl.when(jnp.logical_and(odd, owns(c)))
        def _():
            wb_copy(c).wait_send()

    def down_a(c):
        free_sums(c)
        down(c, 0)

    def middle(c):
        free_sums(c)
        attention_and_up(c)
        down(c, 0)

    def norms_and_project(c):
        norms(c)
        project(c)

    acts = {"W": wait_x, "N": norms_and_project, "Z": attention_and_up, "Y": middle, "a": down_a, "b": lambda c: down(c, 1),
            "s": lambda c: first_sum(c, 0), "t": lambda c: first_sum(c, 1), "x": lambda c: carry(c, 0), "y": lambda c: carry(c, 1), "F": lambda c: finish(c, 0), "G": lambda c: finish(c, 1)}
    order = [(o[0], int(o[1:].rstrip("eo") or 0), {"e": jnp.logical_not(odd), "o": odd}.get(o[-1])) for o in ORDER]

    def guarded(ok, fn, c):
        @pl.when(ok)
        def _():
            fn(c)

    def step(c, carry):
        for name, shift, which in order:
            fn = acts[name]
            if shift < 0:
                ok = c + shift >= 0
                guarded(ok if which is None else jnp.logical_and(ok, which), fn, c + shift)
            elif which is not None:
                guarded(which, fn, c)
            else:
                fn(c)
        return carry

    lax.fori_loop(0, num_chunks, step, 0)
    for c in range(num_chunks, num_chunks + max(-shift for _, shift, _ in order)):
        for name, shift, which in order:
            if shift < 0 and c + shift < num_chunks:
                if which is None:
                    acts[name](jnp.int32(c + shift))
                else:
                    guarded(which, acts[name], jnp.int32(c + shift))

    for c in range(num_chunks - SLOTS, num_chunks):
        c = jnp.int32(c)
        for k in range(2):
            for i in range(TILES):
                p_copy(c, k, i).wait_send()
                s_copy(c, k, i).wait_send()

                @pl.when(jnp.logical_not(last))
                def _():
                    for copy in y_copies(c, k, i, False):
                        copy.wait_send()

                @pl.when(last)
                def _():
                    last_do(c, k, i, lambda copy: copy.wait_send(), lambda copy: copy.wait())

            @pl.when(turning)
            def _():
                c_copy(c, k).wait_send()
    for back in (2, 1):
        c = num_chunks - back * halves + y // per

        @pl.when(jnp.logical_not(jnp.logical_or(first, odd)))
        def _():
            wb_copy(c).wait_send()

    @pl.when(first)
    def _():
        for c in range(halves):
            @pl.when(owns(c))
            def _():
                for copy in x0_copies(jnp.int32(c)):
                    copy.wait_send()

    @pl.when(last)
    def _():
        for i in range(2):
            ref = gbuf.at[pl.ds(0, seqs - 1), pl.ds(0, seq_len - shard)]
            rcopy(ref, ref, g_send.at[i], g_send.at[i], others[0], stage).wait_send()
        for k in range(2):
            @pl.when(jnp.logical_or(per == 1, share(y, k) != lax.rem(y, per)))
            def _():
                arrived(out_ref.at[0, :, :, pl.ds(0, sb), col[k]], out_sem.at[k])

    @pl.when(jnp.logical_not(last))
    def _():
        arrived(out_ref.at[0], out_sem.at[0])


def copy_kernel(src, dst, held, sems):
    places = [(m, b) for m in range(held.shape[0]) for b in range(held.shape[1])]
    into = [pltpu.make_async_copy(src.at[0, m, b], held.at[m, b], sems.at[0, m, b]) for m, b in places]
    out_of = [pltpu.make_async_copy(held.at[m, b], dst.at[0, m, b], sems.at[1, m, b]) for m, b in places]
    for copy in into:
        copy.start()
    for first, second in zip(into, out_of):
        first.wait()
        second.start()
    for copy in out_of:
        copy.wait()


def solution(mesh):
    stages, rows = mesh.shape["pp"], mesh.shape["tp"]

    def stage_body(x_in, ln_params, w_q, w_k, w_v, w_o, w_up, w_down):
        num_micro, batch, shard, d_model = x_in.shape
        heads, hd = w_k.shape[2:]
        ff = w_up.shape[2]
        attn = heads * hd
        seq_len = shard * rows
        chunk = seq_len // HALVES
        num_chunks = num_micro * batch * HALVES
        sb = chunk // 2
        half = d_model // 2
        w_qkv = [w.reshape(d_model * heads, hd) for w in (w_q, w_k, w_v)]
        cos_tab, sin_tab = rope_tables(seq_len, hd)
        dims = (stages, rows, batch, seq_len, chunk, d_model, heads, hd, ff)
        hbm = pl.BlockSpec(memory_space=pl.ANY)
        vmem = pl.BlockSpec(memory_space=pltpu.VMEM)
        dma = pltpu.SemaphoreType.DMA
        out = pl.pallas_call(
            functools.partial(pipeline_kernel, dims),
            out_shape=(jax.ShapeDtypeStruct((1,) + x_in.shape, BF16), jax.ShapeDtypeStruct((num_micro * batch, seq_len, d_model), BF16)),
            in_specs=[hbm, vmem, vmem, vmem] + [hbm] * 6,
            out_specs=(hbm, hbm),
            scratch_shapes=[
                pltpu.VMEM((3, d_model * heads, hd), BF16),
                pltpu.VMEM((d_model, 3 * attn), BF16),
                pltpu.VMEM((d_model, ff), BF16),
                pltpu.VMEM((attn + ff, d_model), BF16),
                pltpu.VMEM((num_chunks, chunk, d_model), BF16),
                pltpu.VMEM((SLOTS, 2, sb, half), BF16),
                pltpu.VMEM((SLOTS, chunk, d_model), BF16),
                pltpu.VMEM((SLOTS, 2, sb, half), BF16),
                pltpu.VMEM((num_chunks, 2, sb, half), BF16),
                pltpu.VMEM((num_chunks, 2, sb, half), BF16),
                pltpu.VMEM((chunk, d_model), BF16),
                pltpu.VMEM((chunk, d_model), BF16),
                pltpu.VMEM((2, chunk, hd), F32),
                pltpu.VMEM((chunk, attn + ff), BF16),
                pltpu.VMEM((chunk, attn), BF16),
                pltpu.VMEM((seq_len, attn), BF16),
                pltpu.VMEM((seq_len, attn), BF16),
                dma((6,)),
                dma((num_chunks,)),
                dma((num_chunks, 2)),
                dma((num_chunks, 2, TILES)),
                dma((num_chunks, 2)),
                dma((2,)),
                dma((rows - 1,)),
                dma((num_micro * batch,)),
                dma((2,)),
                dma((2,)),
                dma((SLOTS, 2, TILES)),
                dma((SLOTS, 2, TILES)),
                dma((SLOTS, 2, TILES, 2)),
                dma((SLOTS, 2, TILES)),
                dma((SLOTS, 2)),
            ],
            compiler_params=pltpu.CompilerParams(collective_id=0, has_side_effects=True, vmem_limit_bytes=67_000_000),
        )(x_in, ln_params[0], cos_tab, sin_tab, *w_qkv, w_o.reshape(attn, d_model), w_up[0], w_down[0])[0]
        return pl.pallas_call(
            copy_kernel, in_specs=[hbm], out_specs=hbm, out_shape=jax.ShapeDtypeStruct(out.shape, out.dtype),
            scratch_shapes=[pltpu.VMEM(out.shape[1:], BF16), dma((2, num_micro, batch))])(out)

    in_specs = (P(None, "dp", "tp", None), P("pp", None, None), P("pp", None, "tp", None, None), P("pp", None, "tp", None), P("pp", None, "tp", None), P("pp", "tp", None, None, None), P("pp", None, "tp"), P("pp", "tp", None))
    return jax.shard_map(stage_body, mesh=mesh, in_specs=in_specs, out_specs=P("pp", None, "dp", "tp", None), check_vma=False)
```

```python
import functools

import jax
import jax.numpy as jnp
import numpy as np
from jax import lax
from jax.experimental import pallas as pl
from jax.experimental.pallas import tpu as pltpu
from jax.sharding import PartitionSpec as P

LN_EPS = 1e-5
ROPE_BASE = 10000.0
MESH = pl.DeviceIdType.MESH
F32 = jnp.float32
BF16 = jnp.bfloat16
COL_TILE = 512
TILES = 2
HALVES = 2
SLOTS = 2
DIRECT = 8
STEP = 0
ORDER = ("W", "N", "s-1", "t-1", "Ye", "Zo", "x-2o", "ao", "y-2o", "b", "F-1", "G-1")
LN_ROWS = 16


def rope_tables(seq_len, head_dim):
    positions = np.arange(seq_len, dtype=np.float32)
    inv_freq = np.float32(ROPE_BASE) ** (np.float32(-2.0) * np.arange(head_dim // 2, dtype=np.float32) / np.float32(head_dim))
    angles = positions[:, None] * inv_freq[None, :]
    cos_tab, sin_tab = np.cos(angles), np.sin(angles)
    return np.concatenate([cos_tab, cos_tab], axis=1), np.concatenate([-sin_tab, sin_tab], axis=1)


def pipeline_kernel(dims, x_in, ln_par, cos_ref, sin_ref, wq_hbm, wk_hbm, wv_hbm, wo_hbm, wup_hbm, wdn_hbm, out_ref, gbuf,
                    raw, wqkv, wup, wod, xbuf, yst, pst, sst, rec1, rec2, ha, hm, stat, act, qs, kc, vc,
                    w_sem, x_sem, one_sem, two_sem, cr_sem, out_sem, x0_send, g_sem, g_send, wb_send, p_send, s_send, y_send, l_send, c_send):
    stages, rows, batch, seq_len, chunk, d_model, heads, hd, ff = dims
    halves = seq_len // chunk
    num_chunks = x_in.shape[0] * batch * halves
    seqs = num_chunks // halves
    half = d_model // 2
    tile = half // TILES
    attn = heads * hd
    shard = seq_len // rows
    per = rows // halves
    sb = chunk // 2

    stage = lax.axis_index("pp")
    y = lax.axis_index("tp")
    first = stage == 0
    last = stage == stages - 1
    nxt = jnp.minimum(stage + 1, stages - 1)
    prv = jnp.maximum(stage - 1, 0)
    others = [lax.rem(y + shift, rows) for shift in sorted(range(1, rows), key=lambda n: min(n, rows - n))]
    odd = lax.rem(stage, 2) == 1
    turning = jnp.logical_and(odd, jnp.logical_not(last))
    direct = DIRECT + STEP * (stage // 2)

    flip, mirror = y + 1 - 2 * lax.rem(y, 2), rows - 1 - y
    partner, cross = (flip, mirror), (mirror, flip)

    def share(row, k):
        return row // 2 if k == 0 else jnp.where(jnp.logical_or(row == 1, row == 2), 1, 0)

    def tokens(index):
        return pl.ds(pl.multiple_of(index * sb, sb), sb)

    def rows_of(row):
        return pl.ds(pl.multiple_of(row * shard, shard), shard)

    def within(row):
        return rows_of(lax.rem(row, per))

    col = (pl.ds(0, half), pl.ds(half, half))

    def rcopy(src, dst, send, recv, row, stg):
        return pltpu.make_async_remote_copy(src_ref=src, dst_ref=dst, send_sem=send, recv_sem=recv,
                                            device_id={"tp": row, "pp": stg}, device_id_type=MESH)

    def arrived(ref, sem):
        rcopy(ref, ref, sem, sem, others[0], stage).wait_recv()

    places = [(src, raw.at[i]) for i, src in enumerate((wq_hbm, wk_hbm, wv_hbm))]
    places += [(wup_hbm, wup), (wo_hbm, wod.at[pl.ds(0, attn)]), (wdn_hbm, wod.at[pl.ds(attn, ff)])]
    weights = [pltpu.make_async_copy(src, dst, w_sem.at[i]) for i, (src, dst) in enumerate(places)]
    for copy in weights:
        copy.start()

    barrier = pltpu.get_barrier_semaphore()
    for row in others:
        pl.semaphore_signal(barrier, inc=1, device_id={"tp": row}, device_id_type=MESH)

    @pl.when(jnp.logical_not(first))
    def _():
        for row in range(rows):
            pl.semaphore_signal(barrier, inc=1, device_id={"tp": row, "pp": prv}, device_id_type=MESH)

    @pl.when(jnp.logical_not(last))
    def _():
        for row in range(rows):
            pl.semaphore_signal(barrier, inc=1, device_id={"tp": row, "pp": nxt}, device_id_type=MESH)

    @pl.when(jnp.logical_or(first, last))
    def _():
        pl.semaphore_signal(barrier, inc=1, device_id={"tp": y, "pp": jnp.where(first, stages - 1, 0)}, device_id_type=MESH)
        pl.semaphore_wait(barrier, 2 * rows)

    @pl.when(jnp.logical_not(jnp.logical_or(first, last)))
    def _():
        pl.semaphore_wait(barrier, 3 * rows - 1)

    def seq_of(c):
        sigma = c // halves
        return sigma // batch, lax.rem(sigma, batch)

    my_rows = within(y)

    def owns(c):
        return y // per == lax.rem(c, halves)

    def x0_local(c):
        m, b = seq_of(c)
        return pltpu.make_async_copy(x_in.at[m, b], xbuf.at[c, my_rows], x_sem.at[c])

    def x0_copies(c):
        m, b = seq_of(c)
        return [rcopy(x_in.at[m, b], xbuf.at[c, my_rows], x0_send.at[i], x_sem.at[c], row, stage) for i, row in enumerate(others)]

    def g_exchange(sigma):
        m, b = sigma // batch, sigma % batch
        return [rcopy(x_in.at[m, b], gbuf.at[sigma, rows_of(y)], g_send.at[0], g_sem.at[sigma], row, stage) for row in others]

    def g_pass(sigma):
        out = []
        for row in others:
            c = sigma * halves + row // per
            out.append(rcopy(gbuf.at[sigma, rows_of(row)], xbuf.at[c, within(row)], g_send.at[1], x_sem.at[c], y, 0))
        return out

    def x0_start(c):
        @pl.when(owns(c))
        def _():
            for copy in x0_copies(jnp.int32(c)):
                copy.start()

    def feed():
        @pl.when(first)
        def _():
            x0_start(0)
            for c in range(num_chunks):
                @pl.when(owns(c))
                def _():
                    x0_local(jnp.int32(c)).start()

        @pl.when(last)
        def _():
            for sigma in range(1, seqs):
                for copy in g_exchange(sigma):
                    copy.start()

    def pass_on():
        @pl.when(last)
        def _():
            for sigma in range(1, seqs):
                arrived(gbuf.at[sigma, pl.ds(0, seq_len - shard)], g_sem.at[sigma])
                for copy in g_pass(sigma):
                    copy.start()

    def wb_copy(c):
        m, b = seq_of(c)
        return rcopy(xbuf.at[c, my_rows], out_ref.at[0, m, b], wb_send.at[lax.rem(c // halves, 2)], out_sem.at[0], y, prv)

    def wait_x(c):
        arrived(xbuf.at[c], x_sem.at[c])

        @pl.when(jnp.logical_and(jnp.logical_not(first), owns(c)))
        def _():
            @pl.when(jnp.logical_and(c >= 2 * halves, jnp.logical_not(odd)))
            def _():
                wb_copy(c - 2 * halves).wait_send()
            wb_copy(c).start()

    def piece(k, i):
        return pl.ds(k * half + i * tile, tile)

    def p_copy(c, k, i):
        p = lax.rem(c, SLOTS)
        return rcopy(pst.at[p, tokens(share(cross[k], k)), piece(k, i)], rec1.at[c, k, :, piece(0, i)],
                     p_send.at[p, k, i], one_sem.at[c, k], cross[k], stage)

    def s_copy(c, k, i):
        p = lax.rem(c, SLOTS)
        return rcopy(sst.at[p, k, :, piece(0, i)], rec2.at[c, k, :, piece(0, i)], s_send.at[p, k, i], two_sem.at[c, k, i], partner[k], stage)

    def first_sum(c, k):
        p = lax.rem(c, SLOTS)

        @pl.when(c >= SLOTS)
        def _():
            for i in range(TILES):
                s_copy(c - SLOTS, k, i).wait_send()
        arrived(rec1.at[c, k], one_sem.at[c, k])
        own = pst[p, tokens(share(y, k)), col[k]]
        sst[p, k] = (rec1[c, k].astype(F32) + own.astype(F32)).astype(BF16)
        for i in range(TILES):
            s_copy(c, k, i).start()

    def y_copies(c, k, i, around):
        p = lax.rem(c, SLOTS)
        src, where = yst.at[p, k, :, piece(0, i)], (c, tokens(share(y, k)), piece(k, i))
        side = rcopy(src, xbuf.at[where], y_send.at[p, k, i, 0], cr_sem.at[c, k, i] if around else x_sem.at[c], cross[k], stage if around else nxt)
        return [side, rcopy(src, xbuf.at[where], y_send.at[p, k, i, 1], x_sem.at[c], y, nxt)]

    def c_copy(c, k, i):
        ref = xbuf.at[c, tokens(share(cross[k], k)), piece(k, i)]
        return rcopy(ref, ref, c_send.at[lax.rem(c, SLOTS), k, i], x_sem.at[c], y, nxt)

    def carry(c, i):
        @pl.when(jnp.logical_and(turning, c >= direct))
        def _():
            for k in range(2):
                @pl.when(c >= direct + SLOTS)
                def _():
                    c_copy(c - SLOTS, k, i).wait_send()
                arrived(xbuf.at[c, tokens(share(cross[k], k)), piece(k, i)], cr_sem.at[c, k, i])
                c_copy(c, k, i).start()

    def last_place(c, k, i):
        token = lax.rem(c, halves) * chunk + share(y, k) * sb
        start = pl.multiple_of(lax.rem(token, shard), sb)
        m, b = seq_of(c)
        return token // shard, out_ref.at[0, m, b, pl.ds(start, sb), piece(k, i)]

    def last_do(c, k, i, remote, local):
        p = lax.rem(c, SLOTS)
        row, dst = last_place(c, k, i)
        src, sem = yst.at[p, k, :, piece(0, i)], l_send.at[p, k, i]

        @pl.when(row == cross[k])
        def _():
            remote(rcopy(src, dst, sem, out_sem.at[k], cross[k], stage))

        @pl.when(row == y)
        def _():
            local(pltpu.make_async_copy(src, dst, sem))

    def finish(c, i):
        p = lax.rem(c, SLOTS)
        around = jnp.logical_and(turning, c >= direct)
        for k in range(2):
            @pl.when(jnp.logical_and(c >= SLOTS, jnp.logical_not(last)))
            def _():
                for copy in y_copies(c - SLOTS, k, i, False):
                    copy.wait_send()

            @pl.when(jnp.logical_and(c >= SLOTS, last))
            def _():
                last_do(c - SLOTS, k, i, lambda copy: copy.wait_send(), lambda copy: copy.wait())
            arrived(rec2.at[c, k, :, piece(0, i)], two_sem.at[c, k, i])
            total = sst[p, k, :, piece(0, i)].astype(F32) + rec2[c, k, :, piece(0, i)].astype(F32)
            yst[p, k, :, piece(0, i)] = (xbuf[c, tokens(share(y, k)), piece(k, i)].astype(F32) + total).astype(BF16)

            @pl.when(around)
            def _():
                for copy in y_copies(c, k, i, True):
                    copy.start()

            @pl.when(jnp.logical_not(jnp.logical_or(around, last)))
            def _():
                for copy in y_copies(c, k, i, False):
                    copy.start()

            @pl.when(last)
            def _():
                last_do(c, k, i, lambda copy: copy.start(), lambda copy: copy.start())

    lanes = stat.shape[2]

    def norms(c):
        gain, bias = ln_par[0:1, :], ln_par[1:2, :]
        for start in range(0, chunk, LN_ROWS):
            part = pl.ds(start, LN_ROWS)
            x = xbuf[c, part].astype(F32)
            mean = jnp.mean(x, axis=-1, keepdims=True)
            centred = x - mean
            scale = lax.rsqrt(jnp.mean(centred * centred, axis=-1, keepdims=True) + LN_EPS)
            ha[part] = (centred * scale * gain + bias).astype(BF16)
            stat[0, part] = jnp.broadcast_to(mean, (LN_ROWS, lanes))
            stat[1, part] = jnp.broadcast_to(scale, (LN_ROWS, lanes))

    def second_norms(c, begin, end):
        for start in range(begin, end, LN_ROWS):
            part = pl.ds(start, LN_ROWS)
            mean, scale = stat[0, part], stat[1, part]
            for left in range(0, d_model, lanes):
                cols = slice(left, left + lanes)
                hm[part, cols] = ((xbuf[c, part, cols].astype(F32) - mean) * scale * ln_par[2:3, cols] + ln_par[3:4, cols]).astype(BF16)

    def project(c):
        start = pl.multiple_of(lax.rem(c, halves) * chunk, chunk)
        where = pl.ds(start, chunk)
        cos, sin = cos_ref[where], sin_ref[where]

        def rope(val):
            turned = jnp.concatenate([val[:, hd // 2:], val[:, :hd // 2]], axis=1)
            return (val * cos + turned * sin).astype(BF16)

        h = ha[...]
        q = jnp.dot(h, wqkv[:, 0:attn], preferred_element_type=F32)
        for i in range(heads):
            qs[:, i * hd:(i + 1) * hd] = rope(q[:, i * hd:(i + 1) * hd])
        second_norms(c, 0, chunk // 2)
        k = jnp.dot(h, wqkv[:, attn:2 * attn], preferred_element_type=F32)
        for i in range(heads):
            kc[where, i * hd:(i + 1) * hd] = rope(k[:, i * hd:(i + 1) * hd])
        second_norms(c, chunk // 2, chunk)
        vc[where, :] = jnp.dot(h, wqkv[:, 2 * attn:3 * attn], preferred_element_type=F32).astype(BF16)

    def attend(c, i):
        row_pos = lax.rem(c, halves) * chunk + lax.broadcasted_iota(jnp.int32, (chunk, seq_len), 0)
        allowed = row_pos >= lax.broadcasted_iota(jnp.int32, (chunk, seq_len), 1)
        cols = slice(i * hd, (i + 1) * hd)
        scores = lax.dot_general(qs[:, cols], kc[:, cols], (((1,), (1,)), ((), ())), preferred_element_type=F32) * (hd ** -0.5)
        scores = jnp.where(allowed, scores, -1e30)
        weights_ = jnp.exp(scores - jnp.max(scores, axis=-1, keepdims=True))
        return (weights_ / jnp.sum(weights_, axis=-1, keepdims=True)).astype(BF16)

    def contract(i, probs):
        cols = slice(i * hd, (i + 1) * hd)
        act[:, cols] = jnp.dot(probs, vc[:, cols], preferred_element_type=F32).astype(BF16)

    def up_tile(i, width):
        cols = slice(i * width, (i + 1) * width)
        u = jnp.dot(hm[...], wup[:, cols], preferred_element_type=F32)
        act[:, attn + i * width:attn + (i + 1) * width] = (0.5 * u * (1.0 + lax.erf(u * np.float32(0.5 ** 0.5)))).astype(BF16)

    def attention_and_up(c):
        for i in range(heads):
            probs = attend(c, i)
            up_tile(i, ff // heads)
            contract(i, probs)

    def down(c, i):
        p = lax.rem(c, SLOTS)
        a = act[...]
        for k in range(2):
            cols = slice(k * half + i * tile, k * half + (i + 1) * tile)
            pst[p, :, cols] = jnp.dot(a, wod[:, cols], preferred_element_type=F32).astype(BF16)
        for k in range(2):
            p_copy(c, k, i).start()

    kc[...] = jnp.zeros_like(kc)
    vc[...] = jnp.zeros_like(vc)
    feed()

    depth = hd // 2
    group = depth * heads
    out_row, in_row = (lax.broadcasted_iota(jnp.int32, (group, group), axis) for axis in (0, 1))
    pick = (in_row == heads * lax.rem(out_row, depth) + out_row // depth).astype(F32).astype(BF16)
    for copy in weights[:3]:
        copy.wait()

    def sort_heads(j, carry):
        rows_in = pl.ds(pl.multiple_of(j * group, group), group)
        rows_out = pl.ds(pl.multiple_of(j * depth, depth), depth)
        pair = jnp.dot(pick, jnp.concatenate([raw[0, rows_in], raw[1, rows_in]], axis=1), preferred_element_type=F32).astype(BF16)
        alone = jnp.dot(pick, raw[2, rows_in], preferred_element_type=F32).astype(BF16)
        for i, val in enumerate((pair[:, :hd], pair[:, hd:], alone)):
            for h in range(heads):
                wqkv[rows_out, i * attn + h * hd:i * attn + (h + 1) * hd] = val[h * depth:(h + 1) * depth]
        return carry

    lax.fori_loop(0, d_model // depth, sort_heads, 0, unroll=4)
    @pl.when(first)
    def _():
        for c in range(1, halves):
            x0_start(c)
    pass_on()
    for copy in weights[3:]:
        copy.wait()

    def free_sums(c):
        @pl.when(c >= SLOTS)
        def _():
            for k in range(2):
                for i in range(TILES):
                    p_copy(c - SLOTS, k, i).wait_send()

        @pl.when(jnp.logical_and(odd, owns(c)))
        def _():
            wb_copy(c).wait_send()

    def down_a(c):
        free_sums(c)
        down(c, 0)

    def middle(c):
        free_sums(c)
        attention_and_up(c)
        down(c, 0)

    def norms_and_project(c):
        norms(c)
        project(c)

    acts = {"W": wait_x, "N": norms_and_project, "Z": attention_and_up, "Y": middle, "a": down_a, "b": lambda c: down(c, 1),
            "s": lambda c: first_sum(c, 0), "t": lambda c: first_sum(c, 1), "x": lambda c: carry(c, 0), "y": lambda c: carry(c, 1), "F": lambda c: finish(c, 0), "G": lambda c: finish(c, 1)}
    order = [(o[0], int(o[1:].rstrip("eo") or 0), {"e": jnp.logical_not(odd), "o": odd}.get(o[-1])) for o in ORDER]

    def guarded(ok, fn, c):
        @pl.when(ok)
        def _():
            fn(c)

    def step(c, carry):
        for name, shift, which in order:
            fn = acts[name]
            if shift < 0:
                ok = c + shift >= 0
                guarded(ok if which is None else jnp.logical_and(ok, which), fn, c + shift)
            elif which is not None:
                guarded(which, fn, c)
            else:
                fn(c)
        return carry

    lax.fori_loop(0, num_chunks, step, 0)
    for c in range(num_chunks, num_chunks + max(-shift for _, shift, _ in order)):
        for name, shift, which in order:
            if shift < 0 and c + shift < num_chunks:
                if which is None:
                    acts[name](jnp.int32(c + shift))
                else:
                    guarded(which, acts[name], jnp.int32(c + shift))

    for c in range(num_chunks - SLOTS, num_chunks):
        c = jnp.int32(c)
        for k in range(2):
            for i in range(TILES):
                p_copy(c, k, i).wait_send()
                s_copy(c, k, i).wait_send()

                @pl.when(jnp.logical_not(last))
                def _():
                    for copy in y_copies(c, k, i, False):
                        copy.wait_send()

                @pl.when(last)
                def _():
                    last_do(c, k, i, lambda copy: copy.wait_send(), lambda copy: copy.wait())

            @pl.when(turning)
            def _():
                for i in range(TILES):
                    c_copy(c, k, i).wait_send()
    for back in (2, 1):
        c = num_chunks - back * halves + y // per

        @pl.when(jnp.logical_not(jnp.logical_or(first, odd)))
        def _():
            wb_copy(c).wait_send()

    @pl.when(first)
    def _():
        for c in range(halves):
            @pl.when(owns(c))
            def _():
                for copy in x0_copies(jnp.int32(c)):
                    copy.wait_send()

    @pl.when(last)
    def _():
        for i in range(2):
            ref = gbuf.at[pl.ds(0, seqs - 1), pl.ds(0, seq_len - shard)]
            rcopy(ref, ref, g_send.at[i], g_send.at[i], others[0], stage).wait_send()
        for k in range(2):
            @pl.when(jnp.logical_or(per == 1, share(y, k) != lax.rem(y, per)))
            def _():
                arrived(out_ref.at[0, :, :, pl.ds(0, sb), col[k]], out_sem.at[k])

    @pl.when(jnp.logical_not(last))
    def _():
        arrived(out_ref.at[0], out_sem.at[0])


def copy_kernel(src, dst, held, sems):
    places = [(m, b) for m in range(held.shape[0]) for b in range(held.shape[1])]
    into = [pltpu.make_async_copy(src.at[0, m, b], held.at[m, b], sems.at[0, m, b]) for m, b in places]
    out_of = [pltpu.make_async_copy(held.at[m, b], dst.at[0, m, b], sems.at[1, m, b]) for m, b in places]
    for copy in into:
        copy.start()
    for first, second in zip(into, out_of):
        first.wait()
        second.start()
    for copy in out_of:
        copy.wait()


def solution(mesh):
    stages, rows = mesh.shape["pp"], mesh.shape["tp"]

    def stage_body(x_in, ln_params, w_q, w_k, w_v, w_o, w_up, w_down):
        num_micro, batch, shard, d_model = x_in.shape
        heads, hd = w_k.shape[2:]
        ff = w_up.shape[2]
        attn = heads * hd
        seq_len = shard * rows
        chunk = seq_len // HALVES
        num_chunks = num_micro * batch * HALVES
        sb = chunk // 2
        half = d_model // 2
        w_qkv = [w.reshape(d_model * heads, hd) for w in (w_q, w_k, w_v)]
        cos_tab, sin_tab = rope_tables(seq_len, hd)
        dims = (stages, rows, batch, seq_len, chunk, d_model, heads, hd, ff)
        hbm = pl.BlockSpec(memory_space=pl.ANY)
        vmem = pl.BlockSpec(memory_space=pltpu.VMEM)
        dma = pltpu.SemaphoreType.DMA
        out = pl.pallas_call(
            functools.partial(pipeline_kernel, dims),
            out_shape=(jax.ShapeDtypeStruct((1,) + x_in.shape, BF16), jax.ShapeDtypeStruct((num_micro * batch, seq_len, d_model), BF16)),
            in_specs=[hbm, vmem, vmem, vmem] + [hbm] * 6,
            out_specs=(hbm, hbm),
            scratch_shapes=[
                pltpu.VMEM((3, d_model * heads, hd), BF16),
                pltpu.VMEM((d_model, 3 * attn), BF16),
                pltpu.VMEM((d_model, ff), BF16),
                pltpu.VMEM((attn + ff, d_model), BF16),
                pltpu.VMEM((num_chunks, chunk, d_model), BF16),
                pltpu.VMEM((SLOTS, 2, sb, half), BF16),
                pltpu.VMEM((SLOTS, chunk, d_model), BF16),
                pltpu.VMEM((SLOTS, 2, sb, half), BF16),
                pltpu.VMEM((num_chunks, 2, sb, half), BF16),
                pltpu.VMEM((num_chunks, 2, sb, half), BF16),
                pltpu.VMEM((chunk, d_model), BF16),
                pltpu.VMEM((chunk, d_model), BF16),
                pltpu.VMEM((2, chunk, hd), F32),
                pltpu.VMEM((chunk, attn + ff), BF16),
                pltpu.VMEM((chunk, attn), BF16),
                pltpu.VMEM((seq_len, attn), BF16),
                pltpu.VMEM((seq_len, attn), BF16),
                dma((6,)),
                dma((num_chunks,)),
                dma((num_chunks, 2)),
                dma((num_chunks, 2, TILES)),
                dma((num_chunks, 2, TILES)),
                dma((2,)),
                dma((rows - 1,)),
                dma((num_micro * batch,)),
                dma((2,)),
                dma((2,)),
                dma((SLOTS, 2, TILES)),
                dma((SLOTS, 2, TILES)),
                dma((SLOTS, 2, TILES, 2)),
                dma((SLOTS, 2, TILES)),
                dma((SLOTS, 2, TILES)),
            ],
            compiler_params=pltpu.CompilerParams(collective_id=0, has_side_effects=True, vmem_limit_bytes=67_000_000),
        )(x_in, ln_params[0], cos_tab, sin_tab, *w_qkv, w_o.reshape(attn, d_model), w_up[0], w_down[0])[0]
        return pl.pallas_call(
            copy_kernel, in_specs=[hbm], out_specs=hbm, out_shape=jax.ShapeDtypeStruct(out.shape, out.dtype),
            scratch_shapes=[pltpu.VMEM(out.shape[1:], BF16), dma((2, num_micro, batch))])(out)

    in_specs = (P(None, "dp", "tp", None), P("pp", None, None), P("pp", None, "tp", None, None), P("pp", None, "tp", None), P("pp", None, "tp", None), P("pp", "tp", None, None, None), P("pp", None, "tp"), P("pp", "tp", None))
    return jax.shard_map(stage_body, mesh=mesh, in_specs=in_specs, out_specs=P("pp", None, "dp", "tp", None), check_vma=False)
```

```python
import functools

import jax
import jax.numpy as jnp
import numpy as np
from jax import lax
from jax.experimental import pallas as pl
from jax.experimental.pallas import tpu as pltpu
from jax.sharding import PartitionSpec as P

LN_EPS = 1e-5
ROPE_BASE = 10000.0
MESH = pl.DeviceIdType.MESH
F32 = jnp.float32
BF16 = jnp.bfloat16
COL_TILE = 512
TILES = 2
HALVES = 2
SLOTS = 2
DIRECT = 8
STEP = 0
ORDER = ("W", "N", "s-1", "t-1", "Ye", "Zo", "x-2o", "ao", "y-2o", "b", "F-1", "G-1")
LN_ROWS = 16


def rope_tables(seq_len, head_dim):
    positions = np.arange(seq_len, dtype=np.float32)
    inv_freq = np.float32(ROPE_BASE) ** (np.float32(-2.0) * np.arange(head_dim // 2, dtype=np.float32) / np.float32(head_dim))
    angles = positions[:, None] * inv_freq[None, :]
    cos_tab, sin_tab = np.cos(angles), np.sin(angles)
    return np.concatenate([cos_tab, cos_tab], axis=1), np.concatenate([-sin_tab, sin_tab], axis=1)


def pipeline_kernel(dims, x_in, ln_par, cos_ref, sin_ref, wq_hbm, wk_hbm, wv_hbm, wo_hbm, wup_hbm, wdn_hbm, out_ref, gbuf,
                    raw, wqkv, wup, wod, xbuf, yst, pst, sst, rec1, rec2, ha, hm, stat, act, qs, kc, vc,
                    w_sem, x_sem, one_sem, two_sem, cr_sem, out_sem, x0_send, g_sem, g_send, wb_send, p_send, s_send, y_send, l_send, c_send):
    stages, rows, batch, seq_len, chunk, d_model, heads, hd, ff = dims
    halves = seq_len // chunk
    num_chunks = x_in.shape[0] * batch * halves
    seqs = num_chunks // halves
    half = d_model // 2
    tile = half // TILES
    attn = heads * hd
    shard = seq_len // rows
    per = rows // halves
    sb = chunk // 2

    stage = lax.axis_index("pp")
    y = lax.axis_index("tp")
    first = stage == 0
    last = stage == stages - 1
    nxt = jnp.minimum(stage + 1, stages - 1)
    prv = jnp.maximum(stage - 1, 0)
    others = [lax.rem(y + shift, rows) for shift in sorted(range(1, rows), key=lambda n: min(n, rows - n))]
    odd = lax.rem(stage, 2) == 1
    turning = jnp.logical_and(odd, jnp.logical_not(last))
    direct = DIRECT + STEP * (stage // 2)

    flip, mirror = y + 1 - 2 * lax.rem(y, 2), rows - 1 - y
    partner, cross = (flip, mirror), (mirror, flip)

    def share(row, k):
        return row // 2 if k == 0 else jnp.where(jnp.logical_or(row == 1, row == 2), 1, 0)

    def tokens(index):
        return pl.ds(pl.multiple_of(index * sb, sb), sb)

    def rows_of(row):
        return pl.ds(pl.multiple_of(row * shard, shard), shard)

    def within(row):
        return rows_of(lax.rem(row, per))

    col = (pl.ds(0, half), pl.ds(half, half))

    def rcopy(src, dst, send, recv, row, stg):
        return pltpu.make_async_remote_copy(src_ref=src, dst_ref=dst, send_sem=send, recv_sem=recv,
                                            device_id={"tp": row, "pp": stg}, device_id_type=MESH)

    def arrived(ref, sem):
        rcopy(ref, ref, sem, sem, others[0], stage).wait_recv()

    places = [(src, raw.at[i]) for i, src in enumerate((wq_hbm, wk_hbm, wv_hbm))]
    places += [(wup_hbm, wup), (wo_hbm, wod.at[pl.ds(0, attn)]), (wdn_hbm, wod.at[pl.ds(attn, ff)])]
    weights = [pltpu.make_async_copy(src, dst, w_sem.at[i]) for i, (src, dst) in enumerate(places)]
    for copy in weights:
        copy.start(priority=1)

    barrier = pltpu.get_barrier_semaphore()
    for row in others:
        pl.semaphore_signal(barrier, inc=1, device_id={"tp": row}, device_id_type=MESH)

    @pl.when(jnp.logical_not(first))
    def _():
        for row in range(rows):
            pl.semaphore_signal(barrier, inc=1, device_id={"tp": row, "pp": prv}, device_id_type=MESH)

    @pl.when(jnp.logical_not(last))
    def _():
        for row in range(rows):
            pl.semaphore_signal(barrier, inc=1, device_id={"tp": row, "pp": nxt}, device_id_type=MESH)

    @pl.when(jnp.logical_or(first, last))
    def _():
        pl.semaphore_signal(barrier, inc=1, device_id={"tp": y, "pp": jnp.where(first, stages - 1, 0)}, device_id_type=MESH)
        pl.semaphore_wait(barrier, 2 * rows)

    @pl.when(jnp.logical_not(jnp.logical_or(first, last)))
    def _():
        pl.semaphore_wait(barrier, 3 * rows - 1)

    def seq_of(c):
        sigma = c // halves
        return sigma // batch, lax.rem(sigma, batch)

    my_rows = within(y)

    def owns(c):
        return y // per == lax.rem(c, halves)

    def x0_local(c):
        m, b = seq_of(c)
        return pltpu.make_async_copy(x_in.at[m, b], xbuf.at[c, my_rows], x_sem.at[c])

    def x0_copies(c):
        m, b = seq_of(c)
        return [rcopy(x_in.at[m, b], xbuf.at[c, my_rows], x0_send.at[i], x_sem.at[c], row, stage) for i, row in enumerate(others)]

    def g_exchange(sigma):
        m, b = sigma // batch, sigma % batch
        return [rcopy(x_in.at[m, b], gbuf.at[sigma, rows_of(y)], g_send.at[0], g_sem.at[sigma], row, stage) for row in others]

    def g_pass(sigma):
        out = []
        for row in others:
            c = sigma * halves + row // per
            out.append(rcopy(gbuf.at[sigma, rows_of(row)], xbuf.at[c, within(row)], g_send.at[1], x_sem.at[c], y, 0))
        return out

    def x0_start(c):
        @pl.when(owns(c))
        def _():
            for copy in x0_copies(jnp.int32(c)):
                copy.start()

    def feed():
        @pl.when(first)
        def _():
            x0_start(0)
            for c in range(num_chunks):
                @pl.when(owns(c))
                def _():
                    x0_local(jnp.int32(c)).start()

        @pl.when(last)
        def _():
            for sigma in range(1, seqs):
                for copy in g_exchange(sigma):
                    copy.start()

    def pass_on():
        @pl.when(last)
        def _():
            for sigma in range(1, seqs):
                arrived(gbuf.at[sigma, pl.ds(0, seq_len - shard)], g_sem.at[sigma])
                for copy in g_pass(sigma):
                    copy.start()

    def wb_copy(c):
        m, b = seq_of(c)
        return rcopy(xbuf.at[c, my_rows], out_ref.at[0, m, b], wb_send.at[lax.rem(c // halves, 2)], out_sem.at[0], y, prv)

    def wait_x(c):
        arrived(xbuf.at[c], x_sem.at[c])

        @pl.when(jnp.logical_and(jnp.logical_not(first), owns(c)))
        def _():
            @pl.when(jnp.logical_and(c >= 2 * halves, jnp.logical_not(odd)))
            def _():
                wb_copy(c - 2 * halves).wait_send()
            wb_copy(c).start()

    def piece(k, i):
        return pl.ds(k * half + i * tile, tile)

    def p_copy(c, k, i):
        p = lax.rem(c, SLOTS)
        return rcopy(pst.at[p, tokens(share(cross[k], k)), piece(k, i)], rec1.at[c, k, :, piece(0, i)],
                     p_send.at[p, k, i], one_sem.at[c, k], cross[k], stage)

    def s_copy(c, k, i):
        p = lax.rem(c, SLOTS)
        return rcopy(sst.at[p, k, :, piece(0, i)], rec2.at[c, k, :, piece(0, i)], s_send.at[p, k, i], two_sem.at[c, k, i], partner[k], stage)

    def first_sum(c, k):
        p = lax.rem(c, SLOTS)

        @pl.when(c >= SLOTS)
        def _():
            for i in range(TILES):
                s_copy(c - SLOTS, k, i).wait_send()
        arrived(rec1.at[c, k], one_sem.at[c, k])
        own = pst[p, tokens(share(y, k)), col[k]]
        sst[p, k] = (rec1[c, k].astype(F32) + own.astype(F32)).astype(BF16)
        for i in range(TILES):
            s_copy(c, k, i).start()

    def y_copies(c, k, i, around):
        p = lax.rem(c, SLOTS)
        src, where = yst.at[p, k, :, piece(0, i)], (c, tokens(share(y, k)), piece(k, i))
        side = rcopy(src, xbuf.at[where], y_send.at[p, k, i, 0], cr_sem.at[c, k, i] if around else x_sem.at[c], cross[k], stage if around else nxt)
        return [side, rcopy(src, xbuf.at[where], y_send.at[p, k, i, 1], x_sem.at[c], y, nxt)]

    def c_copy(c, k, i):
        ref = xbuf.at[c, tokens(share(cross[k], k)), piece(k, i)]
        return rcopy(ref, ref, c_send.at[lax.rem(c, SLOTS), k, i], x_sem.at[c], y, nxt)

    def carry(c, i):
        @pl.when(jnp.logical_and(turning, c >= direct))
        def _():
            for k in range(2):
                @pl.when(c >= direct + SLOTS)
                def _():
                    c_copy(c - SLOTS, k, i).wait_send()
                arrived(xbuf.at[c, tokens(share(cross[k], k)), piece(k, i)], cr_sem.at[c, k, i])
                c_copy(c, k, i).start()

    def last_place(c, k, i):
        token = lax.rem(c, halves) * chunk + share(y, k) * sb
        start = pl.multiple_of(lax.rem(token, shard), sb)
        m, b = seq_of(c)
        return token // shard, out_ref.at[0, m, b, pl.ds(start, sb), piece(k, i)]

    def last_do(c, k, i, remote, local):
        p = lax.rem(c, SLOTS)
        row, dst = last_place(c, k, i)
        src, sem = yst.at[p, k, :, piece(0, i)], l_send.at[p, k, i]

        @pl.when(row == cross[k])
        def _():
            remote(rcopy(src, dst, sem, out_sem.at[k], cross[k], stage))

        @pl.when(row == y)
        def _():
            local(pltpu.make_async_copy(src, dst, sem))

    def finish(c, i):
        p = lax.rem(c, SLOTS)
        around = jnp.logical_and(turning, c >= direct)
        for k in range(2):
            @pl.when(jnp.logical_and(c >= SLOTS, jnp.logical_not(last)))
            def _():
                for copy in y_copies(c - SLOTS, k, i, False):
                    copy.wait_send()

            @pl.when(jnp.logical_and(c >= SLOTS, last))
            def _():
                last_do(c - SLOTS, k, i, lambda copy: copy.wait_send(), lambda copy: copy.wait())
            arrived(rec2.at[c, k, :, piece(0, i)], two_sem.at[c, k, i])
            total = sst[p, k, :, piece(0, i)].astype(F32) + rec2[c, k, :, piece(0, i)].astype(F32)
            yst[p, k, :, piece(0, i)] = (xbuf[c, tokens(share(y, k)), piece(k, i)].astype(F32) + total).astype(BF16)

            @pl.when(around)
            def _():
                for copy in y_copies(c, k, i, True):
                    copy.start()

            @pl.when(jnp.logical_not(jnp.logical_or(around, last)))
            def _():
                for copy in y_copies(c, k, i, False):
                    copy.start()

            @pl.when(last)
            def _():
                last_do(c, k, i, lambda copy: copy.start(), lambda copy: copy.start())

    lanes = stat.shape[2]

    def norms(c):
        gain, bias = ln_par[0:1, :], ln_par[1:2, :]
        for start in range(0, chunk, LN_ROWS):
            part = pl.ds(start, LN_ROWS)
            x = xbuf[c, part].astype(F32)
            mean = jnp.mean(x, axis=-1, keepdims=True)
            centred = x - mean
            scale = lax.rsqrt(jnp.mean(centred * centred, axis=-1, keepdims=True) + LN_EPS)
            ha[part] = (centred * scale * gain + bias).astype(BF16)
            stat[0, part] = jnp.broadcast_to(mean, (LN_ROWS, lanes))
            stat[1, part] = jnp.broadcast_to(scale, (LN_ROWS, lanes))

    def second_norms(c, begin, end):
        for start in range(begin, end, LN_ROWS):
            part = pl.ds(start, LN_ROWS)
            mean, scale = stat[0, part], stat[1, part]
            for left in range(0, d_model, lanes):
                cols = slice(left, left + lanes)
                hm[part, cols] = ((xbuf[c, part, cols].astype(F32) - mean) * scale * ln_par[2:3, cols] + ln_par[3:4, cols]).astype(BF16)

    def project(c):
        start = pl.multiple_of(lax.rem(c, halves) * chunk, chunk)
        where = pl.ds(start, chunk)
        cos, sin = cos_ref[where], sin_ref[where]

        def rope(val):
            turned = jnp.concatenate([val[:, hd // 2:], val[:, :hd // 2]], axis=1)
            return (val * cos + turned * sin).astype(BF16)

        h = ha[...]
        q = jnp.dot(h, wqkv[:, 0:attn], preferred_element_type=F32)
        for i in range(heads):
            qs[:, i * hd:(i + 1) * hd] = rope(q[:, i * hd:(i + 1) * hd])
        second_norms(c, 0, chunk // 2)
        k = jnp.dot(h, wqkv[:, attn:2 * attn], preferred_element_type=F32)
        for i in range(heads):
            kc[where, i * hd:(i + 1) * hd] = rope(k[:, i * hd:(i + 1) * hd])
        second_norms(c, chunk // 2, chunk)
        vc[where, :] = jnp.dot(h, wqkv[:, 2 * attn:3 * attn], preferred_element_type=F32).astype(BF16)

    def attend(c, i):
        row_pos = lax.rem(c, halves) * chunk + lax.broadcasted_iota(jnp.int32, (chunk, seq_len), 0)
        allowed = row_pos >= lax.broadcasted_iota(jnp.int32, (chunk, seq_len), 1)
        cols = slice(i * hd, (i + 1) * hd)
        scores = lax.dot_general(qs[:, cols], kc[:, cols], (((1,), (1,)), ((), ())), preferred_element_type=F32) * (hd ** -0.5)
        scores = jnp.where(allowed, scores, -1e30)
        weights_ = jnp.exp(scores - jnp.max(scores, axis=-1, keepdims=True))
        return (weights_ / jnp.sum(weights_, axis=-1, keepdims=True)).astype(BF16)

    def contract(i, probs):
        cols = slice(i * hd, (i + 1) * hd)
        act[:, cols] = jnp.dot(probs, vc[:, cols], preferred_element_type=F32).astype(BF16)

    def up_tile(i, width):
        cols = slice(i * width, (i + 1) * width)
        u = jnp.dot(hm[...], wup[:, cols], preferred_element_type=F32)
        act[:, attn + i * width:attn + (i + 1) * width] = (0.5 * u * (1.0 + lax.erf(u * np.float32(0.5 ** 0.5)))).astype(BF16)

    def attention_and_up(c):
        for i in range(heads):
            probs = attend(c, i)
            up_tile(i, ff // heads)
            contract(i, probs)

    def down(c, i):
        p = lax.rem(c, SLOTS)
        a = act[...]
        for k in range(2):
            cols = slice(k * half + i * tile, k * half + (i + 1) * tile)
            pst[p, :, cols] = jnp.dot(a, wod[:, cols], preferred_element_type=F32).astype(BF16)
        for k in range(2):
            p_copy(c, k, i).start()

    kc[...] = jnp.zeros_like(kc)
    vc[...] = jnp.zeros_like(vc)
    feed()

    depth = hd // 2
    group = depth * heads
    out_row, in_row = (lax.broadcasted_iota(jnp.int32, (group, group), axis) for axis in (0, 1))
    pick = (in_row == heads * lax.rem(out_row, depth) + out_row // depth).astype(F32).astype(BF16)
    for copy in weights[:3]:
        copy.wait()

    def sort_heads(j, carry):
        rows_in = pl.ds(pl.multiple_of(j * group, group), group)
        rows_out = pl.ds(pl.multiple_of(j * depth, depth), depth)
        pair = jnp.dot(pick, jnp.concatenate([raw[0, rows_in], raw[1, rows_in]], axis=1), preferred_element_type=F32).astype(BF16)
        alone = jnp.dot(pick, raw[2, rows_in], preferred_element_type=F32).astype(BF16)
        for i, val in enumerate((pair[:, :hd], pair[:, hd:], alone)):
            for h in range(heads):
                wqkv[rows_out, i * attn + h * hd:i * attn + (h + 1) * hd] = val[h * depth:(h + 1) * depth]
        return carry

    lax.fori_loop(0, d_model // depth, sort_heads, 0, unroll=4)
    @pl.when(first)
    def _():
        for c in range(1, halves):
            x0_start(c)
    pass_on()
    for copy in weights[3:]:
        copy.wait()

    def free_sums(c):
        @pl.when(c >= SLOTS)
        def _():
            for k in range(2):
                for i in range(TILES):
                    p_copy(c - SLOTS, k, i).wait_send()

        @pl.when(jnp.logical_and(odd, owns(c)))
        def _():
            wb_copy(c).wait_send()

    def down_a(c):
        free_sums(c)
        down(c, 0)

    def middle(c):
        free_sums(c)
        attention_and_up(c)
        down(c, 0)

    def norms_and_project(c):
        norms(c)
        project(c)

    acts = {"W": wait_x, "N": norms_and_project, "Z": attention_and_up, "Y": middle, "a": down_a, "b": lambda c: down(c, 1),
            "s": lambda c: first_sum(c, 0), "t": lambda c: first_sum(c, 1), "x": lambda c: carry(c, 0), "y": lambda c: carry(c, 1), "F": lambda c: finish(c, 0), "G": lambda c: finish(c, 1)}
    order = [(o[0], int(o[1:].rstrip("eo") or 0), {"e": jnp.logical_not(odd), "o": odd}.get(o[-1])) for o in ORDER]

    def guarded(ok, fn, c):
        @pl.when(ok)
        def _():
            fn(c)

    def step(c, carry):
        for name, shift, which in order:
            fn = acts[name]
            if shift < 0:
                ok = c + shift >= 0
                guarded(ok if which is None else jnp.logical_and(ok, which), fn, c + shift)
            elif which is not None:
                guarded(which, fn, c)
            else:
                fn(c)
        return carry

    lax.fori_loop(0, num_chunks, step, 0)
    for c in range(num_chunks, num_chunks + max(-shift for _, shift, _ in order)):
        for name, shift, which in order:
            if shift < 0 and c + shift < num_chunks:
                if which is None:
                    acts[name](jnp.int32(c + shift))
                else:
                    guarded(which, acts[name], jnp.int32(c + shift))

    for c in range(num_chunks - SLOTS, num_chunks):
        c = jnp.int32(c)
        for k in range(2):
            for i in range(TILES):
                p_copy(c, k, i).wait_send()
                s_copy(c, k, i).wait_send()

                @pl.when(jnp.logical_not(last))
                def _():
                    for copy in y_copies(c, k, i, False):
                        copy.wait_send()

                @pl.when(last)
                def _():
                    last_do(c, k, i, lambda copy: copy.wait_send(), lambda copy: copy.wait())

            @pl.when(turning)
            def _():
                for i in range(TILES):
                    c_copy(c, k, i).wait_send()
    for back in (2, 1):
        c = num_chunks - back * halves + y // per

        @pl.when(jnp.logical_not(jnp.logical_or(first, odd)))
        def _():
            wb_copy(c).wait_send()

    @pl.when(first)
    def _():
        for c in range(halves):
            @pl.when(owns(c))
            def _():
                for copy in x0_copies(jnp.int32(c)):
                    copy.wait_send()

    @pl.when(last)
    def _():
        for i in range(2):
            ref = gbuf.at[pl.ds(0, seqs - 1), pl.ds(0, seq_len - shard)]
            rcopy(ref, ref, g_send.at[i], g_send.at[i], others[0], stage).wait_send()
        for k in range(2):
            @pl.when(jnp.logical_or(per == 1, share(y, k) != lax.rem(y, per)))
            def _():
                arrived(out_ref.at[0, :, :, pl.ds(0, sb), col[k]], out_sem.at[k])

    @pl.when(jnp.logical_not(last))
    def _():
        arrived(out_ref.at[0], out_sem.at[0])


def copy_kernel(src, dst, held, sems):
    places = [(m, b) for m in range(held.shape[0]) for b in range(held.shape[1])]
    into = [pltpu.make_async_copy(src.at[0, m, b], held.at[m, b], sems.at[0, m, b]) for m, b in places]
    out_of = [pltpu.make_async_copy(held.at[m, b], dst.at[0, m, b], sems.at[1, m, b]) for m, b in places]
    for copy in into:
        copy.start()
    for first, second in zip(into, out_of):
        first.wait()
        second.start()
    for copy in out_of:
        copy.wait()


def solution(mesh):
    stages, rows = mesh.shape["pp"], mesh.shape["tp"]

    def stage_body(x_in, ln_params, w_q, w_k, w_v, w_o, w_up, w_down):
        num_micro, batch, shard, d_model = x_in.shape
        heads, hd = w_k.shape[2:]
        ff = w_up.shape[2]
        attn = heads * hd
        seq_len = shard * rows
        chunk = seq_len // HALVES
        num_chunks = num_micro * batch * HALVES
        sb = chunk // 2
        half = d_model // 2
        w_qkv = [w.reshape(d_model * heads, hd) for w in (w_q, w_k, w_v)]
        cos_tab, sin_tab = rope_tables(seq_len, hd)
        dims = (stages, rows, batch, seq_len, chunk, d_model, heads, hd, ff)
        hbm = pl.BlockSpec(memory_space=pl.ANY)
        vmem = pl.BlockSpec(memory_space=pltpu.VMEM)
        dma = pltpu.SemaphoreType.DMA
        out = pl.pallas_call(
            functools.partial(pipeline_kernel, dims),
            out_shape=(jax.ShapeDtypeStruct((1,) + x_in.shape, BF16), jax.ShapeDtypeStruct((num_micro * batch, seq_len, d_model), BF16)),
            in_specs=[hbm, vmem, vmem, vmem] + [hbm] * 6,
            out_specs=(hbm, hbm),
            scratch_shapes=[
                pltpu.VMEM((3, d_model * heads, hd), BF16),
                pltpu.VMEM((d_model, 3 * attn), BF16),
                pltpu.VMEM((d_model, ff), BF16),
                pltpu.VMEM((attn + ff, d_model), BF16),
                pltpu.VMEM((num_chunks, chunk, d_model), BF16),
                pltpu.VMEM((SLOTS, 2, sb, half), BF16),
                pltpu.VMEM((SLOTS, chunk, d_model), BF16),
                pltpu.VMEM((SLOTS, 2, sb, half), BF16),
                pltpu.VMEM((num_chunks, 2, sb, half), BF16),
                pltpu.VMEM((num_chunks, 2, sb, half), BF16),
                pltpu.VMEM((chunk, d_model), BF16),
                pltpu.VMEM((chunk, d_model), BF16),
                pltpu.VMEM((2, chunk, hd), F32),
                pltpu.VMEM((chunk, attn + ff), BF16),
                pltpu.VMEM((chunk, attn), BF16),
                pltpu.VMEM((seq_len, attn), BF16),
                pltpu.VMEM((seq_len, attn), BF16),
                dma((6,)),
                dma((num_chunks,)),
                dma((num_chunks, 2)),
                dma((num_chunks, 2, TILES)),
                dma((num_chunks, 2, TILES)),
                dma((2,)),
                dma((rows - 1,)),
                dma((num_micro * batch,)),
                dma((2,)),
                dma((2,)),
                dma((SLOTS, 2, TILES)),
                dma((SLOTS, 2, TILES)),
                dma((SLOTS, 2, TILES, 2)),
                dma((SLOTS, 2, TILES)),
                dma((SLOTS, 2, TILES)),
            ],
            compiler_params=pltpu.CompilerParams(collective_id=0, has_side_effects=True, vmem_limit_bytes=67_000_000),
        )(x_in, ln_params[0], cos_tab, sin_tab, *w_qkv, w_o.reshape(attn, d_model), w_up[0], w_down[0])[0]
        return pl.pallas_call(
            copy_kernel, in_specs=[hbm], out_specs=hbm, out_shape=jax.ShapeDtypeStruct(out.shape, out.dtype),
            scratch_shapes=[pltpu.VMEM(out.shape[1:], BF16), dma((2, num_micro, batch))])(out)

    in_specs = (P(None, "dp", "tp", None), P("pp", None, None), P("pp", None, "tp", None, None), P("pp", None, "tp", None), P("pp", None, "tp", None), P("pp", "tp", None, None, None), P("pp", None, "tp"), P("pp", "tp", None))
    return jax.shard_map(stage_body, mesh=mesh, in_specs=in_specs, out_specs=P("pp", None, "dp", "tp", None), check_vma=False)
```
